64 devices in a mesh: data: 4 (over x, y), ctx: 16 (over z, core).
Axes of the slice: x: 2, y: 2, z: 8, core: 2. Of those that a mesh axis runs over, the one named last changes fastest.
The devices are a block of a 4x4x8 slice.
Arguments:
- hidden: bfloat16 [2048, 5120], P(('data', 'ctx')), parts along dimension 0
- seq_lens: int32 [2048], P(('data', 'ctx')), parts along dimension 0
- w_query: bfloat16 [1, 5120, 5120], replicated
- w_key: bfloat16 [1, 5120, 1024], replicated
- w_value: bfloat16 [1, 5120, 1024], replicated
- w_out: bfloat16 [1, 5120, 5120], replicated
- k_prefix: bfloat16 [1, 16384, 8, 128], P(None, ('data', 'ctx')), parts along dimension 1
- v_prefix: bfloat16 [1, 16384, 8, 128], P(None, ('data', 'ctx')), parts along dimension 1
- k_suffix: bfloat16 [1, 2048, 32, 8, 128], P(None, ('data', 'ctx')), parts along dimension 1
- v_suffix: bfloat16 [1, 2048, 32, 8, 128], P(None, ('data', 'ctx')), parts along dimension 1
Outputs:
- output 1: bfloat16 [2048, 5120], P(('data', 'ctx')), parts along dimension 0
- output 2: bfloat16 [1, 2048, 32, 8, 128], P(None, ('data', 'ctx')), parts along dimension 1
- output 3: bfloat16 [1, 2048, 32, 8, 128], P(None, ('data', 'ctx')), parts along dimension 1
There are 4 independent parts. The reference program is written for one: setup_inputs(seed, part) draws one part's arguments, and reference() takes and returns one part's arrays. A program takes and returns all parts, laid end to end along the dimension named above; an argument that names none is the same for every part.
All inputs are finite; a program needn't handle non-finite values.
Results may differ from the reference program's by a relative error of at most 0.007338.
Values are sent between devices in bfloat16 or wider.
A program may use at most 768 MiB of HBM per device.

```python
import jax
import jax.numpy as jnp
from jax import lax

MODEL_DIM = 5120
NUM_HEADS = 40
KV_HEADS = 8
HEAD_DIM = 128
LAYERS = 1
SHARDS = 16
BATCH_SIZE = 512
PREFIX_LEN = 4096
SUFFIX_LEN = 32
HOME_ROWS = 32


def setup_inputs(seed: int = 0, part: int = 0) -> dict:
    shared_keys = jax.random.split(jax.random.key(seed), 4)
    part_keys = jax.random.split(jax.random.fold_in(jax.random.key(seed + 1), part), 10)
    q_width = NUM_HEADS * HEAD_DIM
    kv_width = KV_HEADS * HEAD_DIM
    shard_rows = PREFIX_LEN // SHARDS
    w_query = jax.random.normal(shared_keys[0], (LAYERS, MODEL_DIM, q_width), jnp.float32) * MODEL_DIM ** -0.5
    w_key = jax.random.normal(shared_keys[1], (LAYERS, MODEL_DIM, kv_width), jnp.float32) * (2.5 * MODEL_DIM ** -0.5)
    w_value = jax.random.normal(shared_keys[2], (LAYERS, MODEL_DIM, kv_width), jnp.float32) * MODEL_DIM ** -0.5
    w_out = jax.random.normal(shared_keys[3], (LAYERS, q_width, MODEL_DIM), jnp.float32) * (q_width * LAYERS) ** -0.5
    hidden = jax.random.normal(part_keys[0], (BATCH_SIZE, MODEL_DIM), jnp.float32)
    centre_shape = (LAYERS, SHARDS, 1, KV_HEADS, HEAD_DIM)
    block_shape = (LAYERS, SHARDS, shard_rows, KV_HEADS, HEAD_DIM)
    prefix_shape = (LAYERS, PREFIX_LEN, KV_HEADS, HEAD_DIM)
    k_prefix = (1.5 * jax.random.normal(part_keys[1], centre_shape, jnp.float32) + jax.random.normal(part_keys[2], block_shape, jnp.float32)).reshape(prefix_shape)
    v_prefix = (jax.random.normal(part_keys[3], centre_shape, jnp.float32) + 0.5 * jax.random.normal(part_keys[4], block_shape, jnp.float32)).reshape(prefix_shape)
    seq_centre = (LAYERS, BATCH_SIZE, 1, KV_HEADS, HEAD_DIM)
    suffix_shape = (LAYERS, BATCH_SIZE, SUFFIX_LEN, KV_HEADS, HEAD_DIM)
    k_suffix = 2.5 * jax.random.normal(part_keys[5], seq_centre, jnp.float32) + jax.random.normal(part_keys[6], suffix_shape, jnp.float32)
    v_suffix = jax.random.normal(part_keys[7], seq_centre, jnp.float32) + 0.5 * jax.random.normal(part_keys[8], suffix_shape, jnp.float32)
    len_keys = jax.random.split(part_keys[9], 2)
    seq_lens = jax.random.randint(len_keys[0], (BATCH_SIZE,), 0, SUFFIX_LEN, dtype=jnp.int32)
    longest = jax.random.randint(len_keys[1], (), 0, BATCH_SIZE, dtype=jnp.int32)
    seq_lens = seq_lens.at[longest].set(SUFFIX_LEN - 1)
    seq_lens = seq_lens.at[(longest + BATCH_SIZE // 2) % BATCH_SIZE].set(0)
    return {'hidden': hidden.astype(jnp.bfloat16), 'seq_lens': seq_lens, 'w_query': w_query.astype(jnp.bfloat16), 'w_key': w_key.astype(jnp.bfloat16), 'w_value': w_value.astype(jnp.bfloat16), 'w_out': w_out.astype(jnp.bfloat16), 'k_prefix': k_prefix.astype(jnp.bfloat16), 'v_prefix': v_prefix.astype(jnp.bfloat16), 'k_suffix': k_suffix.astype(jnp.bfloat16), 'v_suffix': v_suffix.astype(jnp.bfloat16)}


def attend_block(queries, k_pre, v_pre, k_suf, v_suf, slot_live):
    score_scale = HEAD_DIM ** -0.5
    pre_scores = jnp.einsum('bkgd,pkd->bkgp', queries, k_pre) * score_scale
    suf_scores = jnp.einsum('bkgd,bskd->bkgs', queries, k_suf) * score_scale
    suf_scores = jnp.where(slot_live[:, None, None, :], suf_scores, -jnp.inf)
    row_max = jnp.maximum(pre_scores.max(axis=-1), suf_scores.max(axis=-1))
    pre_exp = jnp.exp(pre_scores - row_max[..., None])
    suf_exp = jnp.exp(suf_scores - row_max[..., None])
    mass_sum = pre_exp.sum(axis=-1) + suf_exp.sum(axis=-1)
    mixed_sum = jnp.einsum('bkgp,pkd->bkgd', pre_exp, v_pre) + jnp.einsum('bkgs,bskd->bkgd', suf_exp, v_suf)
    return mixed_sum / mass_sum[..., None]


def reference(hidden, seq_lens, w_query, w_key, w_value, w_out, k_prefix, v_prefix, k_suffix, v_suffix):
    group_size = NUM_HEADS // KV_HEADS
    blocks = BATCH_SIZE // HOME_ROWS
    slot_ids = jnp.arange(SUFFIX_LEN, dtype=jnp.int32)[None, :]
    slot_hit = (slot_ids == seq_lens[:, None])[:, :, None, None]
    slot_live = slot_ids <= seq_lens[:, None]
    live_blocks = slot_live.reshape(blocks, HOME_ROWS, SUFFIX_LEN)

    def layer_step(hidden_state, layer_args):
        q_weight, k_weight, v_weight, o_weight, k_pre, v_pre, k_suf, v_suf = layer_args
        queries = jnp.dot(hidden_state, q_weight, preferred_element_type=jnp.float32).astype(jnp.bfloat16)
        k_new = jnp.dot(hidden_state, k_weight, preferred_element_type=jnp.float32).astype(jnp.bfloat16).reshape(BATCH_SIZE, 1, KV_HEADS, HEAD_DIM)
        v_new = jnp.dot(hidden_state, v_weight, preferred_element_type=jnp.float32).astype(jnp.bfloat16).reshape(BATCH_SIZE, 1, KV_HEADS, HEAD_DIM)
        k_suf = jnp.where(slot_hit, k_new, k_suf)
        v_suf = jnp.where(slot_hit, v_new, v_suf)
        q_blocks = queries.astype(jnp.float32).reshape(blocks, HOME_ROWS, KV_HEADS, group_size, HEAD_DIM)
        k_full = k_pre.astype(jnp.float32)
        v_full = v_pre.astype(jnp.float32)
        k_blocks = k_suf.astype(jnp.float32).reshape(blocks, HOME_ROWS, SUFFIX_LEN, KV_HEADS, HEAD_DIM)
        v_blocks = v_suf.astype(jnp.float32).reshape(blocks, HOME_ROWS, SUFFIX_LEN, KV_HEADS, HEAD_DIM)
        attended = lax.map(lambda block_args: attend_block(block_args[0], k_full, v_full, block_args[1], block_args[2], block_args[3]), (q_blocks, k_blocks, v_blocks, live_blocks))
        attended = attended.astype(jnp.bfloat16).reshape(BATCH_SIZE, NUM_HEADS * HEAD_DIM)
        update = jnp.dot(attended, o_weight, preferred_element_type=jnp.float32).astype(jnp.bfloat16)
        hidden_state = (hidden_state.astype(jnp.float32) + update.astype(jnp.float32)).astype(jnp.bfloat16)
        return hidden_state, (k_suf, v_suf)

    hidden_out, cache_out = lax.scan(layer_step, hidden, (w_query, w_key, w_value, w_out, k_prefix, v_prefix, k_suffix, v_suffix))
    return hidden_out, cache_out[0], cache_out[1]
```

```python
import functools
import math

import jax
import jax.numpy as jnp
from jax import lax
from jax.experimental import pallas as pl
from jax.experimental.pallas import tpu as pltpu
from jax.sharding import PartitionSpec as P

MESH = pl.DeviceIdType.MESH
CORES = 2
CHUNK = 512
RING = 3
OUT_SLOTS = 5
UNROLL = 4


def hop_of(step):
    return (step + 1) // 2 * (1 - 2 * ((step + 1) % 2))


def decode_kernel(n, dims, lens, x_hbm, wq, wk, wv, wo, kp, vp, ks_hbm, vs_hbm, out_ref, kn_out,
                  x2, wqb, wkb, wvb, wob, kraw, vraw, tmp, kvsend, kvrecv, acc, qsend, qrecv, qsib, knv_send, knv_recv,
                  q32, kn32, vn32, ksuf, vsuf, suf_o, suf_m, suf_l, scr, osend, lsend, orecv, lrecv, oacc,
                  in_sem, wsem, wosem, x_ssem, x_rsem, kv_ssem, kv_rsem, fw_ssem, q_ssem, q_rsem, sib_ssem, sib_rsem,
                  o_ssem, o_rsem, l_ssem, l_rsem):
    rows, model, heads, group, dim, slots, pre = dims
    chips = n // CORES
    qw = heads * group * dim
    q_half = qw // CORES
    kv_half = heads * dim // CORES
    my_heads = heads // CORES
    qrows = group * rows
    base2 = dim ** -0.5 * math.log2(math.e)
    me = lax.axis_index('ctx')
    chip = me // CORES
    core = me % CORES
    sib = me + 1 - 2 * core
    f32, bf16 = jnp.float32, jnp.bfloat16
    steps = model // CHUNK
    out_rows = qw // chips

    def loads():
        return [
            pltpu.make_async_copy(kp, kraw, in_sem.at[0]),
            pltpu.make_async_copy(vp, vraw, in_sem.at[1]),
            pltpu.make_async_copy(x_hbm, x2.at[core], in_sem.at[2]),
            pltpu.make_async_copy(ks_hbm, ksuf, in_sem.at[3]),
            pltpu.make_async_copy(vs_hbm, vsuf, in_sem.at[4]),
        ]

    def weight_copies(step, slot):
        r = pl.ds(pl.multiple_of(step * CHUNK, CHUNK), CHUNK)
        qc = pl.ds(pl.multiple_of(core * q_half, 128), q_half)
        kc = pl.ds(pl.multiple_of(core * kv_half, 128), kv_half)
        return [
            pltpu.make_async_copy(wq.at[0, r, qc], wqb.at[slot], wsem.at[slot, 0]),
            pltpu.make_async_copy(wk.at[0, r, kc], wkb.at[slot], wsem.at[slot, 1]),
            pltpu.make_async_copy(wv.at[0, r, kc], wvb.at[slot], wsem.at[slot, 2]),
        ]

    def home_of(step):
        return lax.rem(chip + hop_of(step) + chips, chips)

    def head_of(step):
        return lax.rem(chip - hop_of(step) + chips, chips)

    def out_copy(step):
        slot = lax.rem(step, OUT_SLOTS)
        r = pl.ds(pl.multiple_of(head_of(step) * out_rows, out_rows), out_rows)
        return pltpu.make_async_copy(wo.at[0, r, :], wob.at[slot], wosem.at[slot])

    first = loads()
    for c in first[:3]:
        c.start()
    for s in range(RING):
        for c in weight_copies(s, s):
            c.start()

    barrier = pltpu.get_barrier_semaphore()

    @pl.loop(1, n)
    def _(d):
        pl.semaphore_signal(barrier, inc=1, device_id={'ctx': lax.rem(me + d, n)}, device_id_type=MESH)

    for c in first[3:]:
        c.start()
    for part, raw in ((0, kraw), (1, vraw)):
        first[part].wait()
        tmp[...] = raw[...].astype(f32)
        for h in range(heads):
            kvsend[h, part] = tmp[pl.ds(h, pre, stride=heads), :].astype(bf16)
    kvrecv[me] = kvsend[chip]
    acc[...] = jnp.zeros_like(acc)
    first[2].wait()
    pl.semaphore_wait(barrier, n - 1)

    x_copy = pltpu.make_async_remote_copy(x2.at[core], x2.at[core], x_ssem, x_rsem, device_id={'ctx': sib}, device_id_type=MESH)
    x_copy.start()

    def kv_copy(step):
        t = home_of(step)
        return pltpu.make_async_remote_copy(kvsend.at[t], kvrecv.at[me], kv_ssem.at[step], kv_rsem.at[me],
                                            device_id={'ctx': t * CORES + core}, device_id_type=MESH)

    def fw_copy(step):
        j = home_of(step) * CORES + core
        src = kvsend.at[chip] if step == 0 else kvrecv.at[j]
        return pltpu.make_async_remote_copy(src, kvrecv.at[j], fw_ssem.at[step], kv_rsem.at[j],
                                            device_id={'ctx': sib}, device_id_type=MESH)

    def kv_arrival(j):
        return pltpu.make_async_remote_copy(kvsend.at[0], kvrecv.at[j], kv_ssem.at[0], kv_rsem.at[j],
                                            device_id={'ctx': sib}, device_id_type=MESH)

    for step in range(1, chips):
        kv_copy(step).start()
    fw_copy(0).start()
    x_copy.wait()

    @pl.loop(0, steps)
    def _(j):
        slot = lax.rem(j, RING)
        for c in weight_copies(j, slot):
            c.wait()
        xc = x2[:, :, pl.ds(pl.multiple_of(j * CHUNK, CHUNK), CHUNK)].reshape(CORES * rows, CHUNK)
        for b in range(0, q_half, 512):
            acc[:, b:b + 512] += jnp.dot(xc, wqb[slot, :, b:b + 512], preferred_element_type=f32)
        acc[:, q_half:q_half + kv_half] += jnp.dot(xc, wkb[slot], preferred_element_type=f32)
        acc[:, q_half + kv_half:] += jnp.dot(xc, wvb[slot], preferred_element_type=f32)

        @pl.when(j + RING < steps)
        def _():
            for c in weight_copies(j + RING, slot):
                c.start()

        @pl.when(j + RING >= steps)
        def _():
            out_copy(j + RING - steps).start()

    for s in range(RING, OUT_SLOTS):
        out_copy(s).start()

    for hh in range(my_heads * group):
        tl, g = hh // group, hh % group
        block = acc[:, hh * dim:(hh + 1) * dim].astype(bf16)
        for r in range(CORES):
            qsend[r, tl, g * rows:(g + 1) * rows, :] = block[r * rows:(r + 1) * rows]
    for part in range(2):
        for hl in range(my_heads):
            lo = q_half + part * kv_half + hl * dim
            block = acc[:, lo:lo + dim].astype(bf16)
            for r in range(CORES):
                knv_send[r, part, hl * rows:(hl + 1) * rows, :] = block[r * rows:(r + 1) * rows]

    def sib_copies():
        return [
            pltpu.make_async_remote_copy(qsend.at[1 - core], qsib, sib_ssem.at[0], sib_rsem.at[0], device_id={'ctx': sib}, device_id_type=MESH),
            pltpu.make_async_remote_copy(knv_send.at[1 - core], knv_recv, sib_ssem.at[1], sib_rsem.at[1], device_id={'ctx': sib}, device_id_type=MESH),
        ]

    for c in sib_copies():
        c.start()

    def q_copy(tl, r):
        t = core * my_heads + tl
        return pltpu.make_async_remote_copy(qsend.at[r, tl], qrecv.at[chip], q_ssem.at[tl, r], q_rsem.at[chip],
                                            device_id={'ctx': t * CORES + r}, device_id_type=MESH)

    def q_arrival(c):
        return pltpu.make_async_remote_copy(qsend.at[0, 0], qrecv.at[c], q_ssem.at[0, 0], q_rsem.at[c],
                                            device_id={'ctx': sib}, device_id_type=MESH)

    q_is_local = chip // my_heads == core

    @pl.loop(0, my_heads)
    def _(i):
        tl = lax.rem(chip + i, my_heads)
        for r in range(CORES):
            here = jnp.logical_and(core * my_heads + tl == chip, core == r)

            @pl.when(jnp.logical_not(here))
            def _():
                q_copy(tl, r).start()

            @pl.when(here)
            def _():
                qrecv[chip] = qsend[r, tl]

    own = qsend[core].reshape(my_heads * qrows, dim).astype(f32)
    q32[pl.ds(pl.multiple_of(core * my_heads * qrows, 8), my_heads * qrows), :] = own
    own_kv = knv_send[core].astype(f32)
    own_at = pl.ds(pl.multiple_of(core * my_heads * rows, 8), my_heads * rows)
    kn32[own_at, :] = own_kv[0]
    vn32[own_at, :] = own_kv[1]
    for c in sib_copies():
        c.wait()
    sib_at = 1 - core
    q32[pl.ds(pl.multiple_of(sib_at * my_heads * qrows, 8), my_heads * qrows), :] = qsib[...].reshape(my_heads * qrows, dim).astype(f32)
    sib_kv = knv_recv[...].astype(f32)
    other = pl.ds(pl.multiple_of(sib_at * my_heads * rows, 8), my_heads * rows)
    kn32[other, :] = sib_kv[0]
    vn32[other, :] = sib_kv[1]
    kn_out[0] = kn32[...].astype(bf16)
    kn_out[1] = vn32[...].astype(bf16)

    first[3].wait()
    first[4].wait()
    n_q = heads * group
    row_id = lax.broadcasted_iota(jnp.int32, (n_q, slots * heads), 0)
    col_id = lax.broadcasted_iota(jnp.int32, (n_q, slots * heads), 1)
    low = (col_id & (heads - 1)) * group
    same_head = jnp.logical_and(row_id >= low, row_id < low + group)
    slot_of = col_id >> int(math.log2(heads))
    slot3 = lax.broadcasted_iota(jnp.int32, (slots, heads, dim), 0)

    @pl.loop(0, rows // UNROLL)
    def _(i):
        for u in range(UNROLL):
            b = i * UNROLL + u
            length = lens[b]
            qb = q32[pl.ds(b, n_q, stride=rows), :].astype(bf16)
            hit = slot3 == length
            kb = jnp.where(hit, kn32[pl.ds(b, heads, stride=rows), :][None], ksuf[b].astype(f32).reshape(slots, heads, dim))
            vb = jnp.where(hit, vn32[pl.ds(b, heads, stride=rows), :][None], vsuf[b].astype(f32).reshape(slots, heads, dim))
            kb = kb.reshape(slots * heads, dim).astype(bf16)
            vb = vb.reshape(slots * heads, dim).astype(bf16)
            s = lax.dot_general(qb, kb, (((1,), (1,)), ((), ())), preferred_element_type=f32)
            live = jnp.logical_and(same_head, slot_of <= length)
            s = jnp.where(live, s, -jnp.inf)
            m = s.max(axis=-1, keepdims=True)
            p = jnp.where(live, jnp.exp2((s - m) * base2), 0.0)
            l = p.sum(axis=-1, keepdims=True)
            ob = jnp.dot(p.astype(bf16), vb, preferred_element_type=f32)
            at = pl.ds(b, n_q, stride=rows)
            suf_o[at, :] = ob
            suf_m[at, :] = jnp.broadcast_to(m * base2, (n_q, dim))
            suf_l[at, :] = jnp.broadcast_to(l, (n_q, dim))

    for step in range(1, chips):
        kv_arrival(home_of(step) * CORES + core).wait_recv()
        fw_copy(step).start()
    for c in range(chips):
        kv_arrival(c * CORES + 1 - core).wait_recv()

    eye = lax.broadcasted_iota(jnp.int32, (128, 128), 0) == lax.broadcasted_iota(jnp.int32, (128, 128), 1)

    def o_copy(c):
        return pltpu.make_async_remote_copy(osend.at[c], orecv.at[chip], o_ssem.at[c], o_rsem.at[chip],
                                            device_id={'ctx': c * CORES + core}, device_id_type=MESH)

    def l_copy(c):
        return pltpu.make_async_remote_copy(lsend.at[c], lrecv.at[chip], l_ssem.at[c], l_rsem.at[chip],
                                            device_id={'ctx': c * CORES + core}, device_id_type=MESH)

    def o_arrival(t):
        return pltpu.make_async_remote_copy(osend.at[0], orecv.at[t], o_ssem.at[0], o_rsem.at[t],
                                            device_id={'ctx': sib}, device_id_type=MESH)

    def l_arrival(t):
        return pltpu.make_async_remote_copy(lsend.at[0], lrecv.at[t], l_ssem.at[0], l_rsem.at[t],
                                            device_id={'ctx': sib}, device_id_type=MESH)

    @pl.loop(0, chips)
    def _(step):
        c = home_of(step)

        @pl.when(jnp.logical_not(jnp.logical_and(step == 0, q_is_local)))
        def _():
            q_arrival(c).wait_recv()

        q = qrecv[c]
        top = jnp.full((qrows, dim), -jnp.inf, f32)
        for s in range(n):
            sc = lax.dot_general(q, kvrecv[s, 0], (((1,), (1,)), ((), ())), preferred_element_type=f32)
            scr[s] = sc
            for b in range(0, pre, dim):
                top = jnp.maximum(top, sc[:, b:b + dim])
        m = top.max(axis=-1, keepdims=True) * base2
        mass = jnp.zeros((qrows, dim), f32)
        o = jnp.zeros((qrows, dim), f32)
        for s in range(n):
            p = jnp.exp2(scr[s] * base2 - m)
            for b in range(0, pre, dim):
                mass += p[:, b:b + dim]
            o += jnp.dot(p.astype(bf16), kvrecv[s, 1], preferred_element_type=f32)
        l = mass.sum(axis=-1, keepdims=True)
        o = (o / l).astype(bf16)
        lse = jnp.broadcast_to(m + jnp.log2(l), (qrows, dim))
        row0 = jnp.where(eye, lse[:dim], 0.0).sum(axis=0, keepdims=True)
        row1 = jnp.where(eye[:qrows - dim], lse[dim:], 0.0).sum(axis=0, keepdims=True)

        @pl.when(step == 0)
        def _():
            orecv[c] = o
            lrecv[c, 0:1, :] = row0
            lrecv[c, 1:2, :] = row1

        @pl.when(step > 0)
        def _():
            osend[c] = o
            lsend[c] = jnp.zeros_like(lsend[c])
            lsend[c, 0:1, :] = row0
            lsend[c, 1:2, :] = row1
            o_copy(c).start()
            l_copy(c).start()

    oacc[...] = jnp.zeros_like(oacc)

    @pl.loop(0, chips)
    def _(step):
        t = head_of(step)

        @pl.when(step > 0)
        def _():
            o_arrival(t).wait_recv()
            l_arrival(t).wait_recv()

        row0 = jnp.broadcast_to(lrecv[t, 0:1, :], (dim, dim))
        row1 = jnp.broadcast_to(lrecv[t, 1:2, :], (qrows - dim, dim))
        lse = jnp.concatenate([
            jnp.where(eye, row0, 0.0).sum(axis=-1, keepdims=True),
            jnp.where(eye[:qrows - dim], row1, 0.0).sum(axis=-1, keepdims=True),
        ], axis=0)
        at = pl.ds(pl.multiple_of(t * qrows, 8), qrows)
        sm = suf_m[at, :]
        top = jnp.maximum(lse, sm)
        wp = jnp.exp2(lse - top)
        ws = jnp.exp2(sm - top)
        o = (wp * orecv[t].astype(f32) + ws * suf_o[at, :]) / (wp + ws * suf_l[at, :])
        o = o.astype(bf16)
        att = jnp.concatenate([o[g * rows:(g + 1) * rows] for g in range(group)], axis=1)
        out_copy(step).wait()
        slot = lax.rem(step, OUT_SLOTS)
        for b in range(0, model, 512):
            oacc[:, b:b + 512] += jnp.dot(att, wob[slot, :, b:b + 512], preferred_element_type=f32)

        @pl.when(step + OUT_SLOTS < chips)
        def _():
            out_copy(step + OUT_SLOTS).start()

    out_ref[...] = (x2[core].astype(f32) + oacc[...].astype(bf16).astype(f32)).astype(bf16)

    for step in range(1, chips):
        kv_copy(step).wait_send()
    for step in range(chips):
        fw_copy(step).wait_send()

    @pl.loop(0, my_heads)
    def _(tl):
        for r in range(CORES):
            @pl.when(jnp.logical_not(jnp.logical_and(core * my_heads + tl == chip, core == r)))
            def _():
                q_copy(tl, r).wait_send()

    @pl.loop(1, chips)
    def _(step):
        c = home_of(step)
        o_copy(c).wait_send()
        l_copy(c).wait_send()


def solution(mesh):
    n = mesh.shape['ctx']
    home_axes = ('data', 'ctx')
    row_spec = P(home_axes, None)
    lens_spec = P(home_axes)
    whole_spec = P()
    prefix_spec = P(None, home_axes, None, None)
    cache_spec = P(None, home_axes, None, None, None)
    bf16, f32 = jnp.bfloat16, jnp.float32

    def attend(hidden, seq_lens, wq, wk, wv, wo, kp, vp, ks, vs):
        rows, model = hidden.shape
        _, pre, heads, dim = kp.shape
        slots = ks.shape[2]
        group = wq.shape[2] // (heads * dim)
        chips = n // CORES
        my_heads = heads // CORES
        qrows = group * rows
        qw = heads * group * dim
        dims = (rows, model, heads, group, dim, slots, pre)
        dma = pltpu.SemaphoreType.DMA
        vmem = pltpu.VMEM
        scratch = [
            vmem((CORES, rows, model), bf16),
            vmem((RING, CHUNK, qw // CORES), bf16),
            vmem((RING, CHUNK, heads * dim // CORES), bf16),
            vmem((RING, CHUNK, heads * dim // CORES), bf16),
            vmem((OUT_SLOTS, qw // chips, model), bf16),
            vmem((pre * heads, dim), bf16),
            vmem((pre * heads, dim), bf16),
            vmem((pre * heads, dim), f32),
            vmem((heads, 2, pre, dim), bf16),
            vmem((n, 2, pre, dim), bf16),
            vmem((CORES * rows, (qw + 2 * heads * dim) // CORES), f32),
            vmem((CORES, my_heads, qrows, dim), bf16),
            vmem((chips, qrows, dim), bf16),
            vmem((my_heads, qrows, dim), bf16),
            vmem((CORES, 2, my_heads * rows, dim), bf16),
            vmem((2, my_heads * rows, dim), bf16),
            vmem((heads * qrows, dim), f32),
            vmem((heads * rows, dim), f32),
            vmem((heads * rows, dim), f32),
            vmem((rows, slots * heads, dim), bf16),
            vmem((rows, slots * heads, dim), bf16),
            vmem((heads * qrows, dim), f32),
            vmem((heads * qrows, dim), f32),
            vmem((heads * qrows, dim), f32),
            vmem((n, qrows, pre), f32),
            vmem((chips, qrows, dim), bf16),
            vmem((chips, 8, dim), f32),
            vmem((chips, qrows, dim), bf16),
            vmem((chips, 8, dim), f32),
            vmem((rows, model), f32),
            dma((5,)),
            dma((RING, 3)),
            dma((OUT_SLOTS,)),
            dma,
            dma,
            dma((chips,)),
            dma((n,)),
            dma((chips,)),
            dma((my_heads, CORES)),
            dma((chips,)),
            dma((2,)),
            dma((2,)),
            dma((chips,)),
            dma((chips,)),
            dma((chips,)),
            dma((chips,)),
        ]
        any_spec = pl.BlockSpec(memory_space=pl.ANY)
        vmem_spec = pl.BlockSpec(memory_space=pltpu.VMEM)
        return pl.pallas_call(
            functools.partial(decode_kernel, n, dims),
            out_shape=(jax.ShapeDtypeStruct((rows, model), bf16), jax.ShapeDtypeStruct((2, heads * rows, dim), bf16)),
            in_specs=[pl.BlockSpec(memory_space=pltpu.SMEM)] + [any_spec] * 9,
            out_specs=(vmem_spec, vmem_spec),
            scratch_shapes=scratch,
            compiler_params=pltpu.CompilerParams(collective_id=0, has_side_effects=True, vmem_limit_bytes=67_043_328),
        )(seq_lens, hidden, wq, wk, wv, wo, kp.reshape(pre * heads, dim), vp.reshape(pre * heads, dim),
          ks.reshape(rows, slots * heads, dim), vs.reshape(rows, slots * heads, dim))

    def local_step(hidden, seq_lens, wq, wk, wv, wo, kp, vp, ks, vs):
        rows = hidden.shape[0]
        _, _, slots, heads, dim = ks.shape
        out, new = attend(hidden, seq_lens, wq, wk, wv, wo, kp, vp, ks, vs)
        hit = (lax.broadcasted_iota(jnp.int32, (rows, slots), 1) == seq_lens[:, None])[None, :, :, None, None]
        new = new.reshape(2, heads, rows, dim).transpose(0, 2, 1, 3)[:, None, :, None]
        return out, jnp.where(hit, new[0], ks), jnp.where(hit, new[1], vs)

    return jax.shard_map(local_step, mesh=mesh, in_specs=(row_spec, lens_spec, whole_spec, whole_spec, whole_spec, whole_spec, prefix_spec, prefix_spec, cache_spec, cache_spec), out_specs=(row_spec, cache_spec, cache_spec), check_vma=False)
```

```python
import functools
import math

import jax
import jax.numpy as jnp
from jax import lax
from jax.experimental import pallas as pl
from jax.experimental.pallas import tpu as pltpu
from jax.sharding import PartitionSpec as P

MESH = pl.DeviceIdType.MESH
CORES = 2
CHUNK = 512
RING = 3
OUT_SLOTS = 4
TILE = 256
HOME_AFTER = {2: (0, 1), 3: (1, 3), 4: (3, 8)}
UNROLL = 4


def hop_of(step):
    return (step + 1) // 2 * (1 - 2 * ((step + 1) % 2))


def decode_kernel(n, dims, lens, x_hbm, wq, wk, wv, wo, kp, vp, ks_hbm, vs_hbm, out_ref, ks_out, vs_out,
                  x2, wqb, wkb, wvb, wob, kraw, vraw, tmp, kvsend, kvrecv, acc, qsend, qrecv, qsib, knv_send, knv_recv,
                  q32, kn32, vn32, ksuf, vsuf, suf_o, suf_m, suf_l, scr, osend, lsend, orecv, lrecv, oacc,
                  in_sem, out_sem, wsem, wosem, x_ssem, x_rsem, kv_ssem, kv_rsem, fw_ssem, q_ssem, q_rsem, sib_ssem, sib_rsem,
                  o_ssem, o_rsem, l_ssem, l_rsem):
    rows, model, heads, group, dim, slots, pre = dims
    chips = n // CORES
    qw = heads * group * dim
    q_half = qw // CORES
    kv_half = heads * dim // CORES
    my_heads = heads // CORES
    qrows = group * rows
    base2 = dim ** -0.5 * math.log2(math.e)
    me = lax.axis_index('ctx')
    chip = me // CORES
    core = me % CORES
    sib = me + 1 - 2 * core
    f32, bf16 = jnp.float32, jnp.bfloat16
    steps = model // CHUNK
    out_rows = qw // chips

    def loads():
        return [
            pltpu.make_async_copy(kp, kraw, in_sem.at[0]),
            pltpu.make_async_copy(vp, vraw, in_sem.at[1]),
            pltpu.make_async_copy(x_hbm, x2.at[core], in_sem.at[2]),
            pltpu.make_async_copy(ks_hbm, ksuf, in_sem.at[3]),
            pltpu.make_async_copy(vs_hbm, vsuf, in_sem.at[4]),
        ]

    def weight_copies(step, slot):
        r = pl.ds(pl.multiple_of(step * CHUNK, CHUNK), CHUNK)
        qc = pl.ds(pl.multiple_of(core * q_half, 128), q_half)
        kc = pl.ds(pl.multiple_of(core * kv_half, 128), kv_half)
        return [
            pltpu.make_async_copy(wq.at[0, r, qc], wqb.at[slot], wsem.at[slot, 0]),
            pltpu.make_async_copy(wk.at[0, r, kc], wkb.at[slot], wsem.at[slot, 1]),
            pltpu.make_async_copy(wv.at[0, r, kc], wvb.at[slot], wsem.at[slot, 2]),
        ]

    def home_of(step):
        return lax.rem(chip + hop_of(step) + chips, chips)

    def head_of(step):
        return lax.rem(chip - hop_of(step) + chips, chips)

    def out_copy(step):
        slot = lax.rem(step, OUT_SLOTS)
        r = pl.ds(pl.multiple_of(head_of(step) * out_rows, out_rows), out_rows)
        return pltpu.make_async_copy(wo.at[0, r, :], wob.at[slot], wosem.at[slot])

    first = loads()
    for c in first[:3]:
        c.start()
    for s in range(RING):
        for c in weight_copies(s, s):
            c.start()

    barrier = pltpu.get_barrier_semaphore()

    @pl.loop(1, n)
    def _(d):
        pl.semaphore_signal(barrier, inc=1, device_id={'ctx': lax.rem(me + d, n)}, device_id_type=MESH)

    for c in first[3:]:
        c.start()
    for part, raw in ((0, kraw), (1, vraw)):
        first[part].wait()
        tmp[...] = raw[...].astype(f32)
        for h in range(heads):
            block = tmp[pl.ds(h, pre, stride=heads), :]
            if part == 0:
                kvsend[h, 0] = block.astype(bf16)
            else:
                for lo in range(0, pre, dim):
                    kvsend[h, 1, lo:lo + dim, :] = block[lo:lo + dim].T.astype(bf16)
    kvrecv[me] = kvsend[chip]
    acc[...] = jnp.zeros_like(acc)
    first[2].wait()
    pl.semaphore_wait(barrier, n - 1)

    x_copy = pltpu.make_async_remote_copy(x2.at[core], x2.at[core], x_ssem, x_rsem, device_id={'ctx': sib}, device_id_type=MESH)
    x_copy.start()

    def kv_copy(step):
        t = home_of(step)
        return pltpu.make_async_remote_copy(kvsend.at[t], kvrecv.at[me], kv_ssem.at[step], kv_rsem.at[me],
                                            device_id={'ctx': t * CORES + core}, device_id_type=MESH)

    def fw_copy(step):
        j = home_of(step) * CORES + core
        src = kvsend.at[chip] if step == 0 else kvrecv.at[j]
        return pltpu.make_async_remote_copy(src, kvrecv.at[j], fw_ssem.at[step], kv_rsem.at[j],
                                            device_id={'ctx': sib}, device_id_type=MESH)

    def kv_arrival(j):
        return pltpu.make_async_remote_copy(kvsend.at[0], kvrecv.at[j], kv_ssem.at[0], kv_rsem.at[j],
                                            device_id={'ctx': sib}, device_id_type=MESH)

    for step in range(1, chips):
        kv_copy(step).start()
    fw_copy(0).start()
    x_copy.wait()

    @pl.loop(0, steps)
    def _(j):
        slot = lax.rem(j, RING)
        for c in weight_copies(j, slot):
            c.wait()
        xc = x2[:, :, pl.ds(pl.multiple_of(j * CHUNK, CHUNK), CHUNK)].reshape(CORES * rows, CHUNK)
        for b in range(0, q_half, 512):
            acc[:, b:b + 512] += jnp.dot(xc, wqb[slot, :, b:b + 512], preferred_element_type=f32)
        acc[:, q_half:q_half + kv_half] += jnp.dot(xc, wkb[slot], preferred_element_type=f32)
        acc[:, q_half + kv_half:] += jnp.dot(xc, wvb[slot], preferred_element_type=f32)

        @pl.when(j + RING < steps)
        def _():
            for c in weight_copies(j + RING, slot):
                c.start()

        @pl.when(j + RING >= steps)
        def _():
            out_copy(j + RING - steps).start()

    for s in range(RING, OUT_SLOTS):
        out_copy(s).start()

    for hh in range(my_heads * group):
        tl, g = hh // group, hh % group
        block = acc[:, hh * dim:(hh + 1) * dim].astype(bf16)
        for r in range(CORES):
            qsend[r, tl, g * rows:(g + 1) * rows, :] = block[r * rows:(r + 1) * rows]
    for part in range(2):
        for hl in range(my_heads):
            lo = q_half + part * kv_half + hl * dim
            block = acc[:, lo:lo + dim].astype(bf16)
            for r in range(CORES):
                knv_send[r, part, hl * rows:(hl + 1) * rows, :] = block[r * rows:(r + 1) * rows]

    def sib_copies():
        return [
            pltpu.make_async_remote_copy(qsend.at[1 - core], qsib, sib_ssem.at[0], sib_rsem.at[0], device_id={'ctx': sib}, device_id_type=MESH),
            pltpu.make_async_remote_copy(knv_send.at[1 - core], knv_recv, sib_ssem.at[1], sib_rsem.at[1], device_id={'ctx': sib}, device_id_type=MESH),
        ]

    for c in sib_copies():
        c.start()

    def place(step):
        return pl.ds(pl.multiple_of(step * qrows, 16), qrows)

    def q_copy(step, r):
        t = head_of(step)
        return pltpu.make_async_remote_copy(qsend.at[r, lax.rem(t, my_heads)], qrecv.at[place(step), :], q_ssem.at[step, r], q_rsem.at[step],
                                            device_id={'ctx': t * CORES + r}, device_id_type=MESH)

    def q_arrival(step):
        return pltpu.make_async_remote_copy(qsend.at[0, 0], qrecv.at[place(step), :], q_ssem.at[0, 0], q_rsem.at[step],
                                            device_id={'ctx': sib}, device_id_type=MESH)

    q_is_local = chip // my_heads == core

    @pl.when(q_is_local)
    def _():
        qrecv[0:qrows, :] = qsend[core, lax.rem(chip, my_heads)]
        q_copy(0, 1 - core).start()

    @pl.loop(1, chips)
    def _(step):
        @pl.when(head_of(step) // my_heads == core)
        def _():
            for r in range(CORES):
                q_copy(step, r).start()

    own = qsend[core].reshape(my_heads * qrows, dim).astype(f32)
    q32[pl.ds(pl.multiple_of(core * my_heads * qrows, 8), my_heads * qrows), :] = own
    own_kv = knv_send[core].astype(f32)
    own_at = pl.ds(pl.multiple_of(core * my_heads * rows, 8), my_heads * rows)
    kn32[own_at, :] = own_kv[0]
    vn32[own_at, :] = own_kv[1]
    for c in sib_copies():
        c.wait()
    sib_at = 1 - core
    q32[pl.ds(pl.multiple_of(sib_at * my_heads * qrows, 8), my_heads * qrows), :] = qsib[...].reshape(my_heads * qrows, dim).astype(f32)
    sib_kv = knv_recv[...].astype(f32)
    other = pl.ds(pl.multiple_of(sib_at * my_heads * rows, 8), my_heads * rows)
    kn32[other, :] = sib_kv[0]
    vn32[other, :] = sib_kv[1]

    first[3].wait()
    first[4].wait()
    n_q = heads * group
    row_id = lax.broadcasted_iota(jnp.int32, (n_q, slots * heads), 0)
    col_id = lax.broadcasted_iota(jnp.int32, (n_q, slots * heads), 1)
    low = (col_id & (heads - 1)) * group
    same_head = jnp.logical_and(row_id >= low, row_id < low + group)
    slot_of = col_id >> int(math.log2(heads))
    slot3 = lax.broadcasted_iota(jnp.int32, (slots, heads, dim), 0)

    @pl.loop(0, rows // UNROLL)
    def _(i):
        for u in range(UNROLL):
            b = i * UNROLL + u
            length = lens[b]
            qb = q32[pl.ds(b, n_q, stride=rows), :].astype(bf16)
            hit = slot3 == length
            kb = jnp.where(hit, kn32[pl.ds(b, heads, stride=rows), :][None], ksuf[b].astype(f32).reshape(slots, heads, dim))
            vb = jnp.where(hit, vn32[pl.ds(b, heads, stride=rows), :][None], vsuf[b].astype(f32).reshape(slots, heads, dim))
            kb = kb.reshape(slots * heads, dim).astype(bf16)
            vb = vb.reshape(slots * heads, dim).astype(bf16)
            ksuf[b] = kb
            vsuf[b] = vb
            s = lax.dot_general(qb, kb, (((1,), (1,)), ((), ())), preferred_element_type=f32)
            live = jnp.logical_and(same_head, slot_of <= length)
            s = jnp.where(live, s, -jnp.inf)
            m = s.max(axis=-1, keepdims=True)
            p = jnp.where(live, jnp.exp2((s - m) * base2), 0.0)
            l = p.sum(axis=-1, keepdims=True)
            ob = jnp.dot(p.astype(bf16), vb, preferred_element_type=f32)
            at = pl.ds(b, n_q, stride=rows)
            suf_o[at, :] = ob
            suf_m[at, :] = jnp.broadcast_to(m * base2, (n_q, dim))
            suf_l[at, :] = jnp.broadcast_to(l, (n_q, dim))

    cache_out = [pltpu.make_async_copy(ksuf, ks_out, out_sem.at[0]), pltpu.make_async_copy(vsuf, vs_out, out_sem.at[1])]
    for c in cache_out:
        c.start()

    for step in range(1, chips):
        kv_arrival(home_of(step) * CORES + core).wait_recv()
        fw_copy(step).start()
    for c in range(chips):
        kv_arrival(c * CORES + 1 - core).wait_recv()

    def o_copy(step):
        return pltpu.make_async_remote_copy(osend.at[place(step), :], orecv.at[step], o_ssem.at[step], o_rsem.at[step],
                                            device_id={'ctx': home_of(step) * CORES + core}, device_id_type=MESH)

    def l_copy(step):
        at = step * qrows // dim
        return pltpu.make_async_remote_copy(lsend.at[pl.ds(at, 2)], lrecv.at[step], l_ssem.at[step], l_rsem.at[step],
                                            device_id={'ctx': home_of(step) * CORES + core}, device_id_type=MESH)

    def scores(tile, s, top):
        q = qrecv[tile * TILE:(tile + 1) * TILE, :]
        sc = lax.dot_general(kvrecv[s, 0], q, (((1,), (1,)), ((), ())), preferred_element_type=f32)
        scr[tile % 2, s] = sc
        return jnp.maximum(top, sc.reshape(pre // 8, 8, TILE).max(axis=0))

    def values(tile, s, m, mass, o):
        p = jnp.exp2(scr[tile % 2, s] * base2 - m)
        mass += p.reshape(pre // 8, 8, TILE).sum(axis=0)
        vt = jnp.concatenate([kvrecv[s, 1, lo:lo + dim, :] for lo in range(0, pre, dim)], axis=1)
        return mass, o + jnp.dot(vt, p.astype(bf16), preferred_element_type=f32)

    lowest = jnp.full((8, TILE), -jnp.inf, f32)
    tiles = chips * qrows // TILE
    row_of = lax.broadcasted_iota(jnp.int32, (qrows, 2 * dim), 0)
    lane_of = lax.broadcasted_iota(jnp.int32, (qrows, 2 * dim), 1)
    oacc[...] = jnp.zeros_like(oacc)

    def home(step):
        @pl.when(step > 0)
        def _():
            o_copy(step).wait_recv()
            l_copy(step).wait_recv()

        t = head_of(step)
        line = jnp.concatenate([lrecv[step, 0], lrecv[step, 1]], axis=1)
        pick = lane_of == row_of + lax.rem(step * qrows, dim)
        lse = jnp.where(pick, jnp.broadcast_to(line, (qrows, 2 * dim)), 0.0).sum(axis=-1, keepdims=True)
        at = pl.ds(pl.multiple_of(t * qrows, 8), qrows)
        sm = suf_m[at, :]
        top = jnp.maximum(lse, sm)
        wp = jnp.exp2(lse - top)
        ws = jnp.exp2(sm - top)
        o = (wp * orecv[step].astype(f32) + ws * suf_o[at, :]) / (wp + ws * suf_l[at, :])
        o = o.astype(bf16)
        att = jnp.concatenate([o[g * rows:(g + 1) * rows] for g in range(group)], axis=1)
        out_copy(step).wait()
        slot = lax.rem(step, OUT_SLOTS)
        for b in range(0, model, 512):
            oacc[:, b:b + 512] += jnp.dot(att, wob[slot, :, b:b + 512], preferred_element_type=f32)

        @pl.when(step + OUT_SLOTS < chips)
        def _():
            out_copy(step + OUT_SLOTS).start()

    tops = None
    arrived = 0
    sent = 0
    for tile in range(tiles + 1):
        if tile < tiles:
            while arrived * qrows < (tile + 1) * TILE:
                if arrived == 0:
                    @pl.when(jnp.logical_not(q_is_local))
                    def _():
                        q_arrival(0).wait_recv()
                else:
                    q_arrival(arrived).wait_recv()
                arrived += 1
        m = None if tile == 0 else tops.max(axis=0, keepdims=True) * base2
        tops = lowest
        mass = jnp.zeros((8, TILE), f32)
        o = jnp.zeros((dim, TILE), f32)
        for s in range(n):
            if tile < tiles:
                tops = scores(tile, s, tops)
            if tile > 0:
                mass, o = values(tile - 1, s, m, mass, o)
        if tile > 0:
            done = tile - 1
            l = mass.sum(axis=0, keepdims=True)
            o = o / l
            lse = m + jnp.log2(l)
            osend[done * TILE:(done + 1) * TILE, :] = o.T.astype(bf16)
            for lo in range(0, TILE, dim):
                lsend[(done * TILE + lo) // dim] = lse[:, lo:lo + dim]
            while (sent + 1) * qrows <= (done + 1) * TILE:
                if sent == 0:
                    orecv[0] = osend[0:qrows, :]
                    lrecv[0] = lsend[0:2]
                else:
                    o_copy(sent).start()
                    l_copy(sent).start()
                sent += 1
            if done in HOME_AFTER:
                pl.loop(*HOME_AFTER[done])(home)

    out_ref[...] = (x2[core].astype(f32) + oacc[...].astype(bf16).astype(f32)).astype(bf16)

    for step in range(1, chips):
        kv_copy(step).wait_send()
    for step in range(chips):
        fw_copy(step).wait_send()

    @pl.when(q_is_local)
    def _():
        q_copy(0, 1 - core).wait_send()

    @pl.loop(1, chips)
    def _(step):
        @pl.when(head_of(step) // my_heads == core)
        def _():
            for r in range(CORES):
                q_copy(step, r).wait_send()
        o_copy(step).wait_send()
        l_copy(step).wait_send()

    for c in cache_out:
        c.wait()


def solution(mesh):
    n = mesh.shape['ctx']
    home_axes = ('data', 'ctx')
    row_spec = P(home_axes, None)
    lens_spec = P(home_axes)
    whole_spec = P()
    prefix_spec = P(None, home_axes, None, None)
    cache_spec = P(None, home_axes, None, None, None)
    bf16, f32 = jnp.bfloat16, jnp.float32

    def attend(hidden, seq_lens, wq, wk, wv, wo, kp, vp, ks, vs):
        rows, model = hidden.shape
        _, pre, heads, dim = kp.shape
        slots = ks.shape[2]
        group = wq.shape[2] // (heads * dim)
        chips = n // CORES
        my_heads = heads // CORES
        qrows = group * rows
        qw = heads * group * dim
        dims = (rows, model, heads, group, dim, slots, pre)
        dma = pltpu.SemaphoreType.DMA
        vmem = pltpu.VMEM
        scratch = [
            vmem((CORES, rows, model), bf16),
            vmem((RING, CHUNK, qw // CORES), bf16),
            vmem((RING, CHUNK, heads * dim // CORES), bf16),
            vmem((RING, CHUNK, heads * dim // CORES), bf16),
            vmem((OUT_SLOTS, qw // chips, model), bf16),
            vmem((pre * heads, dim), bf16),
            vmem((pre * heads, dim), bf16),
            vmem((pre * heads, dim), f32),
            vmem((heads, 2, pre, dim), bf16),
            vmem((n, 2, pre, dim), bf16),
            vmem((CORES * rows, (qw + 2 * heads * dim) // CORES), f32),
            vmem((CORES, my_heads, qrows, dim), bf16),
            vmem((chips * qrows, dim), bf16),
            vmem((my_heads, qrows, dim), bf16),
            vmem((CORES, 2, my_heads * rows, dim), bf16),
            vmem((2, my_heads * rows, dim), bf16),
            vmem((heads * qrows, dim), f32),
            vmem((heads * rows, dim), f32),
            vmem((heads * rows, dim), f32),
            vmem((rows, slots * heads, dim), bf16),
            vmem((rows, slots * heads, dim), bf16),
            vmem((heads * qrows, dim), f32),
            vmem((heads * qrows, dim), f32),
            vmem((heads * qrows, dim), f32),
            vmem((2, n, pre, TILE), f32),
            vmem((chips * qrows, dim), bf16),
            vmem((chips * qrows // dim, 1, dim), f32),
            vmem((chips, qrows, dim), bf16),
            vmem((chips, 2, 1, dim), f32),
            vmem((rows, model), f32),
            dma((5,)),
            dma((2,)),
            dma((RING, 3)),
            dma((OUT_SLOTS,)),
            dma,
            dma,
            dma((chips,)),
            dma((n,)),
            dma((chips,)),
            dma((chips, CORES)),
            dma((chips,)),
            dma((2,)),
            dma((2,)),
            dma((chips,)),
            dma((chips,)),
            dma((chips,)),
            dma((chips,)),
        ]
        any_spec = pl.BlockSpec(memory_space=pl.ANY)
        vmem_spec = pl.BlockSpec(memory_space=pltpu.VMEM)
        return pl.pallas_call(
            functools.partial(decode_kernel, n, dims),
            out_shape=(jax.ShapeDtypeStruct((rows, model), bf16),) + (jax.ShapeDtypeStruct((rows, slots * heads, dim), bf16),) * 2,
            in_specs=[pl.BlockSpec(memory_space=pltpu.SMEM)] + [any_spec] * 9,
            out_specs=(vmem_spec, any_spec, any_spec),
            scratch_shapes=scratch,
            compiler_params=pltpu.CompilerParams(collective_id=0, has_side_effects=True, vmem_limit_bytes=67_043_328),
        )(seq_lens, hidden, wq, wk, wv, wo, kp.reshape(pre * heads, dim), vp.reshape(pre * heads, dim),
          ks.reshape(rows, slots * heads, dim), vs.reshape(rows, slots * heads, dim))

    def local_step(hidden, seq_lens, wq, wk, wv, wo, kp, vp, ks, vs):
        out, k_new, v_new = attend(hidden, seq_lens, wq, wk, wv, wo, kp, vp, ks, vs)
        return out, k_new.reshape(ks.shape), v_new.reshape(vs.shape)

    return jax.shard_map(local_step, mesh=mesh, in_specs=(row_spec, lens_spec, whole_spec, whole_spec, whole_spec, whole_spec, prefix_spec, prefix_spec, cache_spec, cache_spec), out_specs=(row_spec, cache_spec, cache_spec), check_vma=False)
```

```python
import functools
import math

import jax
import jax.numpy as jnp
from jax import lax
from jax.experimental import pallas as pl
from jax.experimental.pallas import tpu as pltpu
from jax.sharding import PartitionSpec as P

MESH = pl.DeviceIdType.MESH
CORES = 2
CHUNK = 512
RING = 3
OUT_SLOTS = 4
TILE = 256
HOME_AFTER = {2: (0, 1), 3: (1, 3), 4: (3, 8)}
UNROLL = 4
SENDS = 2
PIECES = 8


def hop_of(step, chips):
    half = chips // 2
    return (half - step // 2) * (1 - 2 * (step % 2)) + half * ((step + chips - 1) // chips - 1)


def decode_kernel(n, dims, lens, x_hbm, wq, wk, wv, wo, kp, vp, ks_hbm, vs_hbm, out_ref, ks_out, vs_out,
                  x2, wqb, wkb, wvb, wob, kraw, vraw, tmp, kvsend, kvrecv, acc, qsend, qrecv, qsib, knv_send, knv_recv,
                  q32, kn32, vn32, ksuf, vsuf, suf_o, suf_m, suf_l, scr, osend, lsend, orecv, lrecv, oacc,
                  up_sem, in_sem, out_sem, wsem, wosem, x_ssem, x_rsem, kv_ssem, kv_rsem, fw_ssem, q_ssem, q_rsem, sib_ssem, sib_rsem,
                  o_ssem, o_rsem, l_ssem, l_rsem):
    rows, model, heads, group, dim, slots, pre = dims
    chips = n // CORES
    qw = heads * group * dim
    q_half = qw // CORES
    kv_half = heads * dim // CORES
    my_heads = heads // CORES
    qrows = group * rows
    base2 = dim ** -0.5 * math.log2(math.e)
    me = lax.axis_index('ctx')
    chip = me // CORES
    core = me % CORES
    sib = me + 1 - 2 * core
    f32, bf16 = jnp.float32, jnp.bfloat16
    steps = model // CHUNK
    out_rows = qw // chips

    def loads():
        return [
            pltpu.make_async_copy(kp, kraw, in_sem.at[0]),
            pltpu.make_async_copy(vp, vraw, in_sem.at[1]),
            pltpu.make_async_copy(x_hbm, x2.at[core], in_sem.at[2]),
            pltpu.make_async_copy(ks_hbm, ksuf, in_sem.at[3]),
            pltpu.make_async_copy(vs_hbm, vsuf, in_sem.at[4]),
        ]

    def weight_copies(step, slot):
        r = pl.ds(pl.multiple_of(step * CHUNK, CHUNK), CHUNK)
        qc = pl.ds(pl.multiple_of(core * q_half, 128), q_half)
        kc = pl.ds(pl.multiple_of(core * kv_half, 128), kv_half)
        return [
            pltpu.make_async_copy(wq.at[0, r, qc], wqb.at[slot], wsem.at[slot, 0]),
            pltpu.make_async_copy(wk.at[0, r, kc], wkb.at[slot], wsem.at[slot, 1]),
            pltpu.make_async_copy(wv.at[0, r, kc], wvb.at[slot], wsem.at[slot, 2]),
        ]

    def home_of(step):
        return lax.rem(chip + hop_of(step, chips) + chips, chips)

    def head_of(step):
        return lax.rem(chip - hop_of(step, chips) + chips, chips)

    def out_copy(step):
        slot = lax.rem(step, OUT_SLOTS)
        r = pl.ds(pl.multiple_of(head_of(step) * out_rows, out_rows), out_rows)
        return pltpu.make_async_copy(wo.at[0, r, :], wob.at[slot], wosem.at[slot])

    first = loads()
    for c in first[:3]:
        c.start()
    for s in range(RING):
        for c in weight_copies(s, s):
            c.start()

    barrier = pltpu.get_barrier_semaphore()
    pl.semaphore_signal(barrier, inc=1, device_id={'ctx': sib}, device_id_type=MESH)
    for t in range(1, chips):
        @pl.when(t > chip)
        def _():
            for r in range(CORES):
                pl.semaphore_signal(barrier, inc=1, device_id={'ctx': t * CORES + r}, device_id_type=MESH)

    for c in first[3:]:
        c.start()
    for part, raw in ((0, kraw), (1, vraw)):
        first[part].wait()
        tmp[...] = raw[...].astype(f32)
        for h in range(heads):
            block = tmp[pl.ds(h, pre, stride=heads), :]
            if part == 0:
                kvsend[h, 0] = block.astype(bf16)
            else:
                for lo in range(0, pre, dim):
                    kvsend[h, 1, lo:lo + dim, :] = block[lo:lo + dim].T.astype(bf16)
    kvrecv[me] = kvsend[chip]
    first[2].wait()
    pl.semaphore_wait(barrier, chip * CORES + 1)
    for t in range(chips - 1):
        @pl.when(t < chip)
        def _():
            for r in range(CORES):
                pl.semaphore_signal(up_sem.at[chip], inc=1, device_id={'ctx': t * CORES + r}, device_id_type=MESH)

    x_copy = pltpu.make_async_remote_copy(x2.at[core], x2.at[core], x_ssem, x_rsem, device_id={'ctx': sib}, device_id_type=MESH)
    x_copy.start()

    def kv_copy(t):
        return pltpu.make_async_remote_copy(kvsend.at[t], kvrecv.at[me], kv_ssem.at[t], kv_rsem.at[me],
                                            device_id={'ctx': t * CORES + core}, device_id_type=MESH)

    def fw_copy(step):
        j = home_of(step) * CORES + core
        src = kvsend.at[chip] if step == 0 else kvrecv.at[j]
        return pltpu.make_async_remote_copy(src, kvrecv.at[j], fw_ssem.at[step], kv_rsem.at[j],
                                            device_id={'ctx': sib}, device_id_type=MESH)

    def kv_arrival(j):
        return pltpu.make_async_remote_copy(kvsend.at[0], kvrecv.at[j], kv_ssem.at[0], kv_rsem.at[j],
                                            device_id={'ctx': sib}, device_id_type=MESH)

    for step in range(1, chips):
        t = home_of(step)

        @pl.when(t < chip)
        def _():
            kv_copy(t).start()
    fw_copy(0).start()
    acc[...] = jnp.zeros_like(acc)
    x_copy.wait()

    @pl.loop(0, steps)
    def _(j):
        slot = lax.rem(j, RING)
        for c in weight_copies(j, slot):
            c.wait()
        xc = x2[:, :, pl.ds(pl.multiple_of(j * CHUNK, CHUNK), CHUNK)].reshape(CORES * rows, CHUNK)
        for b in range(0, q_half, 512):
            acc[:, b:b + 512] += jnp.dot(xc, wqb[slot, :, b:b + 512], preferred_element_type=f32)
        acc[:, q_half:q_half + kv_half] += jnp.dot(xc, wkb[slot], preferred_element_type=f32)
        acc[:, q_half + kv_half:] += jnp.dot(xc, wvb[slot], preferred_element_type=f32)

        for i in range(SENDS):
            t = chip + 1 + j * SENDS + i

            @pl.when(t < chips)
            def _():
                pl.semaphore_wait(up_sem.at[t], CORES)
                kv_copy(t).start()

        @pl.when(j + RING < steps)
        def _():
            for c in weight_copies(j + RING, slot):
                c.start()

        @pl.when(j + RING >= steps)
        def _():
            out_copy(j + RING - steps).start()

    for s in range(RING, OUT_SLOTS):
        out_copy(s).start()

    for hh in range(my_heads * group):
        tl, g = hh // group, hh % group
        block = acc[:, hh * dim:(hh + 1) * dim].astype(bf16)
        for r in range(CORES):
            qsend[r, tl, g * rows:(g + 1) * rows, :] = block[r * rows:(r + 1) * rows]
    for part in range(2):
        for hl in range(my_heads):
            lo = q_half + part * kv_half + hl * dim
            block = acc[:, lo:lo + dim].astype(bf16)
            for r in range(CORES):
                knv_send[r, part, hl * rows:(hl + 1) * rows, :] = block[r * rows:(r + 1) * rows]

    def sib_copies():
        return [
            pltpu.make_async_remote_copy(qsend.at[1 - core], qsib, sib_ssem.at[0], sib_rsem.at[0], device_id={'ctx': sib}, device_id_type=MESH),
            pltpu.make_async_remote_copy(knv_send.at[1 - core], knv_recv, sib_ssem.at[1], sib_rsem.at[1], device_id={'ctx': sib}, device_id_type=MESH),
        ]

    for c in sib_copies():
        c.start()

    def place(step):
        return pl.ds(pl.multiple_of(step * qrows, 16), qrows)

    def q_copy(step, r):
        t = head_of(step)
        return pltpu.make_async_remote_copy(qsend.at[r, lax.rem(t, my_heads)], qrecv.at[place(step), :], q_ssem.at[step, r], q_rsem.at[step],
                                            device_id={'ctx': t * CORES + r}, device_id_type=MESH)

    def q_arrival(step):
        return pltpu.make_async_remote_copy(qsend.at[0, 0], qrecv.at[place(step), :], q_ssem.at[0, 0], q_rsem.at[step],
                                            device_id={'ctx': sib}, device_id_type=MESH)

    q_is_local = chip // my_heads == core

    @pl.when(q_is_local)
    def _():
        qrecv[0:qrows, :] = qsend[core, lax.rem(chip, my_heads)]
        q_copy(0, 1 - core).start()

    @pl.loop(1, chips)
    def _(step):
        @pl.when(head_of(step) // my_heads == core)
        def _():
            for r in range(CORES):
                q_copy(step, r).start()

    own = qsend[core].reshape(my_heads * qrows, dim).astype(f32)
    q32[pl.ds(pl.multiple_of(core * my_heads * qrows, 8), my_heads * qrows), :] = own
    own_kv = knv_send[core].astype(f32)
    own_at = pl.ds(pl.multiple_of(core * my_heads * rows, 8), my_heads * rows)
    kn32[own_at, :] = own_kv[0]
    vn32[own_at, :] = own_kv[1]
    for c in sib_copies():
        c.wait()
    sib_at = 1 - core
    q32[pl.ds(pl.multiple_of(sib_at * my_heads * qrows, 8), my_heads * qrows), :] = qsib[...].reshape(my_heads * qrows, dim).astype(f32)
    sib_kv = knv_recv[...].astype(f32)
    other = pl.ds(pl.multiple_of(sib_at * my_heads * rows, 8), my_heads * rows)
    kn32[other, :] = sib_kv[0]
    vn32[other, :] = sib_kv[1]

    first[3].wait()
    first[4].wait()
    n_q = heads * group
    row_id = lax.broadcasted_iota(jnp.int32, (n_q, slots * heads), 0)
    col_id = lax.broadcasted_iota(jnp.int32, (n_q, slots * heads), 1)
    low = (col_id & (heads - 1)) * group
    same_head = jnp.logical_and(row_id >= low, row_id < low + group)
    slot_of = col_id >> int(math.log2(heads))
    slot3 = lax.broadcasted_iota(jnp.int32, (slots, heads, dim), 0)

    @pl.loop(0, rows // UNROLL)
    def _(i):
        for u in range(UNROLL):
            b = i * UNROLL + u
            length = lens[b]
            qb = q32[pl.ds(b, n_q, stride=rows), :].astype(bf16)
            hit = slot3 == length
            kb = jnp.where(hit, kn32[pl.ds(b, heads, stride=rows), :][None], ksuf[b].astype(f32).reshape(slots, heads, dim))
            vb = jnp.where(hit, vn32[pl.ds(b, heads, stride=rows), :][None], vsuf[b].astype(f32).reshape(slots, heads, dim))
            kb = kb.reshape(slots * heads, dim).astype(bf16)
            vb = vb.reshape(slots * heads, dim).astype(bf16)
            ksuf[b] = kb
            vsuf[b] = vb
            s = lax.dot_general(qb, kb, (((1,), (1,)), ((), ())), preferred_element_type=f32)
            live = jnp.logical_and(same_head, slot_of <= length)
            s = jnp.where(live, s, -jnp.inf)
            m = s.max(axis=-1, keepdims=True)
            p = jnp.where(live, jnp.exp2((s - m) * base2), 0.0)
            l = p.sum(axis=-1, keepdims=True)
            ob = jnp.dot(p.astype(bf16), vb, preferred_element_type=f32)
            at = pl.ds(b, n_q, stride=rows)
            suf_o[at, :] = ob
            suf_m[at, :] = jnp.broadcast_to(m * base2, (n_q, dim))
            suf_l[at, :] = jnp.broadcast_to(l, (n_q, dim))

    cache_out = [pltpu.make_async_copy(ksuf, ks_out, out_sem.at[0]), pltpu.make_async_copy(vsuf, vs_out, out_sem.at[1])]
    for c in cache_out:
        c.start()

    for step in range(1, chips):
        kv_arrival(home_of(step) * CORES + core).wait_recv()
        fw_copy(step).start()
    for c in range(chips):
        kv_arrival(c * CORES + 1 - core).wait_recv()

    def o_copy(step):
        return pltpu.make_async_remote_copy(osend.at[place(step), :], orecv.at[step], o_ssem.at[step], o_rsem.at[step],
                                            device_id={'ctx': home_of(step) * CORES + core}, device_id_type=MESH)

    def l_copy(step):
        at = step * qrows // dim
        return pltpu.make_async_remote_copy(lsend.at[pl.ds(at, 2)], lrecv.at[step], l_ssem.at[step], l_rsem.at[step],
                                            device_id={'ctx': home_of(step) * CORES + core}, device_id_type=MESH)

    def scores(tile, s, top):
        q = qrecv[tile * TILE:(tile + 1) * TILE, :]
        sc = lax.dot_general(kvrecv[s, 0], q, (((1,), (1,)), ((), ())), preferred_element_type=f32)
        scr[tile % 2, s] = sc
        return jnp.maximum(top, sc.reshape(pre // 8, 8, TILE).max(axis=0))

    def values(tile, s, m, mass, o):
        p = jnp.exp2(scr[tile % 2, s] * base2 - m)
        mass += p.reshape(pre // 8, 8, TILE).sum(axis=0)
        vt = jnp.concatenate([kvrecv[s, 1, lo:lo + dim, :] for lo in range(0, pre, dim)], axis=1)
        return mass, o + jnp.dot(vt, p.astype(bf16), preferred_element_type=f32)

    lowest = jnp.full((8, TILE), -jnp.inf, f32)
    tiles = chips * qrows // TILE
    row_of = lax.broadcasted_iota(jnp.int32, (qrows, 2 * dim), 0)
    lane_of = lax.broadcasted_iota(jnp.int32, (qrows, 2 * dim), 1)
    oacc[...] = jnp.zeros_like(oacc)

    def home(step):
        @pl.when(step > 0)
        def _():
            o_copy(step).wait_recv()
            l_copy(step).wait_recv()

        t = head_of(step)
        line = jnp.concatenate([lrecv[step, 0], lrecv[step, 1]], axis=1)
        pick = lane_of == row_of + lax.rem(step * qrows, dim)
        lse = jnp.where(pick, jnp.broadcast_to(line, (qrows, 2 * dim)), 0.0).sum(axis=-1, keepdims=True)
        at = pl.ds(pl.multiple_of(t * qrows, 8), qrows)
        sm = suf_m[at, :]
        top = jnp.maximum(lse, sm)
        wp = jnp.exp2(lse - top)
        ws = jnp.exp2(sm - top)
        o = (wp * orecv[step].astype(f32) + ws * suf_o[at, :]) / (wp + ws * suf_l[at, :])
        o = o.astype(bf16)
        att = jnp.concatenate([o[g * rows:(g + 1) * rows] for g in range(group)], axis=1)
        out_copy(step).wait()
        slot = lax.rem(step, OUT_SLOTS)
        for b in range(0, model, 512):
            oacc[:, b:b + 512] += jnp.dot(att, wob[slot, :, b:b + 512], preferred_element_type=f32)

        @pl.when(step + OUT_SLOTS < chips)
        def _():
            out_copy(step + OUT_SLOTS).start()

    tops = None
    arrived = 0
    sent = 0
    for tile in range(tiles + 1):
        if tile < tiles:
            while arrived * qrows < (tile + 1) * TILE:
                if arrived == 0:
                    @pl.when(jnp.logical_not(q_is_local))
                    def _():
                        q_arrival(0).wait_recv()
                else:
                    q_arrival(arrived).wait_recv()
                arrived += 1
        m = None if tile == 0 else tops.max(axis=0, keepdims=True) * base2
        tops = lowest
        mass = jnp.zeros((8, TILE), f32)
        o = jnp.zeros((dim, TILE), f32)
        for s in range(n):
            if tile < tiles:
                tops = scores(tile, s, tops)
            if tile > 0:
                mass, o = values(tile - 1, s, m, mass, o)
        if tile > 0:
            done = tile - 1
            l = mass.sum(axis=0, keepdims=True)
            o = o / l
            lse = m + jnp.log2(l)
            osend[done * TILE:(done + 1) * TILE, :] = o.T.astype(bf16)
            for lo in range(0, TILE, dim):
                lsend[(done * TILE + lo) // dim] = lse[:, lo:lo + dim]
            while (sent + 1) * qrows <= (done + 1) * TILE:
                if sent == 0:
                    orecv[0] = osend[0:qrows, :]
                    lrecv[0] = lsend[0:2]
                else:
                    o_copy(sent).start()
                    l_copy(sent).start()
                sent += 1
            if done in HOME_AFTER:
                pl.loop(*HOME_AFTER[done])(home)

    out_ref[...] = (x2[core].astype(f32) + oacc[...].astype(bf16).astype(f32)).astype(bf16)

    for step in range(1, chips):
        kv_copy(home_of(step)).wait_send()
    for step in range(chips):
        fw_copy(step).wait_send()

    @pl.when(q_is_local)
    def _():
        q_copy(0, 1 - core).wait_send()

    @pl.loop(1, chips)
    def _(step):
        @pl.when(head_of(step) // my_heads == core)
        def _():
            for r in range(CORES):
                q_copy(step, r).wait_send()
        o_copy(step).wait_send()
        l_copy(step).wait_send()

    for c in cache_out:
        c.wait()


def publish_kernel(ins, outs, bufs, in_sem, out_sem):
    pieces = []
    for a in range(3):
        count = PIECES if a else 1
        size = ins[a].shape[0] // count
        for i in range(count):
            at = pl.ds(i * size, size)
            k = len(pieces)
            pieces.append((pltpu.make_async_copy(ins[a].at[at], bufs[a].at[at], in_sem.at[k]),
                           pltpu.make_async_copy(bufs[a].at[at], outs[a].at[at], out_sem.at[k])))
    for c, _ in pieces:
        c.start()
    for c, d in pieces:
        c.wait()
        d.start()
    for _, d in pieces:
        d.wait()


def publish(arrays):
    any_spec = pl.BlockSpec(memory_space=pl.ANY)
    count = 1 + 2 * PIECES

    def kernel(a, b, c, x, y, z, p, q, r, in_sem, out_sem):
        publish_kernel((a, b, c), (x, y, z), (p, q, r), in_sem, out_sem)

    return pl.pallas_call(
        kernel,
        out_shape=tuple(jax.ShapeDtypeStruct(a.shape, a.dtype) for a in arrays),
        in_specs=[any_spec] * 3,
        out_specs=(any_spec,) * 3,
        scratch_shapes=[pltpu.VMEM(a.shape, a.dtype) for a in arrays] + [pltpu.SemaphoreType.DMA((count,))] * 2,
        compiler_params=pltpu.CompilerParams(vmem_limit_bytes=67_043_328),
    )(*arrays)


def solution(mesh):
    n = mesh.shape['ctx']
    home_axes = ('data', 'ctx')
    row_spec = P(home_axes, None)
    lens_spec = P(home_axes)
    whole_spec = P()
    prefix_spec = P(None, home_axes, None, None)
    cache_spec = P(None, home_axes, None, None, None)
    bf16, f32 = jnp.bfloat16, jnp.float32

    def attend(hidden, seq_lens, wq, wk, wv, wo, kp, vp, ks, vs):
        rows, model = hidden.shape
        _, pre, heads, dim = kp.shape
        slots = ks.shape[2]
        group = wq.shape[2] // (heads * dim)
        chips = n // CORES
        my_heads = heads // CORES
        qrows = group * rows
        qw = heads * group * dim
        dims = (rows, model, heads, group, dim, slots, pre)
        dma = pltpu.SemaphoreType.DMA
        vmem = pltpu.VMEM
        scratch = [
            vmem((CORES, rows, model), bf16),
            vmem((RING, CHUNK, qw // CORES), bf16),
            vmem((RING, CHUNK, heads * dim // CORES), bf16),
            vmem((RING, CHUNK, heads * dim // CORES), bf16),
            vmem((OUT_SLOTS, qw // chips, model), bf16),
            vmem((pre * heads, dim), bf16),
            vmem((pre * heads, dim), bf16),
            vmem((pre * heads, dim), f32),
            vmem((heads, 2, pre, dim), bf16),
            vmem((n, 2, pre, dim), bf16),
            vmem((CORES * rows, (qw + 2 * heads * dim) // CORES), f32),
            vmem((CORES, my_heads, qrows, dim), bf16),
            vmem((chips * qrows, dim), bf16),
            vmem((my_heads, qrows, dim), bf16),
            vmem((CORES, 2, my_heads * rows, dim), bf16),
            vmem((2, my_heads * rows, dim), bf16),
            vmem((heads * qrows, dim), f32),
            vmem((heads * rows, dim), f32),
            vmem((heads * rows, dim), f32),
            vmem((rows, slots * heads, dim), bf16),
            vmem((rows, slots * heads, dim), bf16),
            vmem((heads * qrows, dim), f32),
            vmem((heads * qrows, dim), f32),
            vmem((heads * qrows, dim), f32),
            vmem((2, n, pre, TILE), f32),
            vmem((chips * qrows, dim), bf16),
            vmem((chips * qrows // dim, 1, dim), f32),
            vmem((chips, qrows, dim), bf16),
            vmem((chips, 2, 1, dim), f32),
            vmem((rows, model), f32),
            pltpu.SemaphoreType.REGULAR((chips,)),
            dma((5,)),
            dma((2,)),
            dma((RING, 3)),
            dma((OUT_SLOTS,)),
            dma,
            dma,
            dma((chips,)),
            dma((n,)),
            dma((chips,)),
            dma((chips, CORES)),
            dma((chips,)),
            dma((2,)),
            dma((2,)),
            dma((chips,)),
            dma((chips,)),
            dma((chips,)),
            dma((chips,)),
        ]
        any_spec = pl.BlockSpec(memory_space=pl.ANY)
        vmem_spec = pl.BlockSpec(memory_space=pltpu.VMEM)
        return pl.pallas_call(
            functools.partial(decode_kernel, n, dims),
            out_shape=(jax.ShapeDtypeStruct((rows, model), bf16),) + (jax.ShapeDtypeStruct((rows, slots * heads, dim), bf16),) * 2,
            in_specs=[pl.BlockSpec(memory_space=pltpu.SMEM)] + [any_spec] * 9,
            out_specs=(vmem_spec, any_spec, any_spec),
            scratch_shapes=scratch,
            compiler_params=pltpu.CompilerParams(collective_id=0, has_side_effects=True, vmem_limit_bytes=67_043_328),
        )(seq_lens, hidden, wq, wk, wv, wo, kp.reshape(pre * heads, dim), vp.reshape(pre * heads, dim),
          ks.reshape(rows, slots * heads, dim), vs.reshape(rows, slots * heads, dim))

    def local_step(hidden, seq_lens, wq, wk, wv, wo, kp, vp, ks, vs):
        out, k_new, v_new = publish(attend(hidden, seq_lens, wq, wk, wv, wo, kp, vp, ks, vs))
        return out, k_new.reshape(ks.shape), v_new.reshape(vs.shape)

    return jax.shard_map(local_step, mesh=mesh, in_specs=(row_spec, lens_spec, whole_spec, whole_spec, whole_spec, whole_spec, prefix_spec, prefix_spec, cache_spec, cache_spec), out_specs=(row_spec, cache_spec, cache_spec), check_vma=False)
```

```python
import functools
import math

import jax
import jax.numpy as jnp
from jax import lax
from jax.experimental import pallas as pl
from jax.experimental.pallas import tpu as pltpu
from jax.sharding import PartitionSpec as P

MESH = pl.DeviceIdType.MESH
CORES = 2
CHUNK = 256
RING = 4
OUT_SLOTS = 5
TILE = 256

UNROLL = 4
PIECES = 8


def hop_of(step, chips):
    half = chips // 2
    return (half - step // 2) * (1 - 2 * (step % 2)) + half * ((step + chips - 1) // chips - 1)


def decode_kernel(n, dims, lens, x_hbm, wq, wk, wv, wo, kp, vp, ks_hbm, vs_hbm, out_ref, ks_out, vs_out,
                  x2, wqb, wkb, wvb, wob, kraw, vraw, tmp, kvsend, kvrecv, acc, qsend, qrecv, qsib, knv_send, knv_recv,
                  q32, kn32, vn32, ksuf, vsuf, suf_o, suf_m, suf_l, scr, osend, lsend, orecv, lrecv, oacc,
                  up_sem, in_sem, out_sem, wsem, wosem, x_ssem, x_rsem, kv_ssem, kv_rsem, fw_ssem, q_ssem, q_rsem, sib_ssem, sib_rsem,
                  o_ssem, o_rsem, l_ssem, l_rsem):
    rows, model, heads, group, dim, slots, pre = dims
    chips = n // CORES
    qw = heads * group * dim
    q_half = qw // CORES
    kv_half = heads * dim // CORES
    my_heads = heads // CORES
    qrows = group * rows
    base2 = dim ** -0.5 * math.log2(math.e)
    me = lax.axis_index('ctx')
    chip = me // CORES
    core = me % CORES
    sib = me + 1 - 2 * core
    f32, bf16 = jnp.float32, jnp.bfloat16
    steps = model // CHUNK
    out_rows = qw // chips

    def loads():
        return [
            pltpu.make_async_copy(kp, kraw, in_sem.at[0]),
            pltpu.make_async_copy(vp, vraw, in_sem.at[1]),
            pltpu.make_async_copy(x_hbm, x2.at[core], in_sem.at[2]),
            pltpu.make_async_copy(ks_hbm, ksuf, in_sem.at[3]),
            pltpu.make_async_copy(vs_hbm, vsuf, in_sem.at[4]),
        ]

    def weight_copies(step, slot):
        r = pl.ds(pl.multiple_of(step * CHUNK, CHUNK), CHUNK)
        qc = pl.ds(pl.multiple_of(core * q_half, 128), q_half)
        kc = pl.ds(pl.multiple_of(core * kv_half, 128), kv_half)
        return [
            pltpu.make_async_copy(wq.at[0, r, qc], wqb.at[slot], wsem.at[slot, 0]),
            pltpu.make_async_copy(wk.at[0, r, kc], wkb.at[slot], wsem.at[slot, 1]),
            pltpu.make_async_copy(wv.at[0, r, kc], wvb.at[slot], wsem.at[slot, 2]),
        ]

    def home_of(step):
        return lax.rem(chip + hop_of(step, chips) + chips, chips)

    def head_of(step):
        return lax.rem(chip - hop_of(step, chips) + chips, chips)

    def near_of(step):
        return lax.rem(chip + (step + 1) // 2 * (1 - 2 * ((step + 1) % 2)) + chips, chips)

    def out_copy(step):
        slot = lax.rem(step, OUT_SLOTS)
        r = pl.ds(pl.multiple_of(head_of(step) * out_rows, out_rows), out_rows)
        return pltpu.make_async_copy(wo.at[0, r, :], wob.at[slot], wosem.at[slot])

    first = loads()
    for c in first[:2]:
        c.start()

    barrier = pltpu.get_barrier_semaphore()
    pl.semaphore_signal(barrier, inc=1, device_id={'ctx': sib}, device_id_type=MESH)
    for t in range(1, chips):
        @pl.when(t > chip)
        def _():
            for r in range(CORES):
                pl.semaphore_signal(barrier, inc=1, device_id={'ctx': t * CORES + r}, device_id_type=MESH)

    pl.semaphore_wait(barrier, chip * CORES + 1)
    for t in range(chips - 1):
        @pl.when(t < chip)
        def _():
            for r in range(CORES):
                pl.semaphore_signal(up_sem.at[chip], inc=1, device_id={'ctx': t * CORES + r}, device_id_type=MESH)

    for part, raw in ((0, kraw), (1, vraw)):
        first[part].wait()
        if part == 1:
            first[2].start()
            for s in range(RING):
                for c in weight_copies(s, s):
                    c.start()
            for c in first[3:]:
                c.start()
        tmp[...] = raw[...].astype(f32)
        for h in range(heads):
            block = tmp[pl.ds(h, pre, stride=heads), :]
            if part == 0:
                kvsend[h, 0] = block.astype(bf16)
            else:
                for lo in range(0, pre, dim):
                    kvsend[h, 1, lo:lo + dim, :] = block[lo:lo + dim].T.astype(bf16)
    kvrecv[me] = kvsend[chip]
    x_copy = pltpu.make_async_remote_copy(x2.at[core], x2.at[core], x_ssem, x_rsem, device_id={'ctx': sib}, device_id_type=MESH)

    def kv_copy(t):
        return pltpu.make_async_remote_copy(kvsend.at[t], kvrecv.at[me], kv_ssem.at[t], kv_rsem.at[me],
                                            device_id={'ctx': t * CORES + core}, device_id_type=MESH)

    def fw_copy(step):
        j = near_of(step) * CORES + core
        src = kvsend.at[chip] if step == 0 else kvrecv.at[j]
        return pltpu.make_async_remote_copy(src, kvrecv.at[j], fw_ssem.at[step], kv_rsem.at[j],
                                            device_id={'ctx': sib}, device_id_type=MESH)

    def kv_arrival(j):
        return pltpu.make_async_remote_copy(kvsend.at[0], kvrecv.at[j], kv_ssem.at[0], kv_rsem.at[j],
                                            device_id={'ctx': sib}, device_id_type=MESH)

    for step in range(1, chips):
        t = near_of(step)

        @pl.when(t > chip)
        def _():
            pl.semaphore_wait(up_sem.at[t], CORES)

        kv_copy(t).start()
    fw_copy(0).start()
    first[2].wait()
    x_copy.start()
    acc[...] = jnp.zeros_like(acc)
    x_copy.wait()

    @pl.loop(0, steps)
    def _(j):
        slot = lax.rem(j, RING)
        for c in weight_copies(j, slot):
            c.wait()
        xc = x2[:, :, pl.ds(pl.multiple_of(j * CHUNK, CHUNK), CHUNK)].reshape(CORES * rows, CHUNK)
        for b in range(0, q_half, 512):
            acc[:, b:b + 512] += jnp.dot(xc, wqb[slot, :, b:b + 512], preferred_element_type=f32)
        acc[:, q_half:q_half + kv_half] += jnp.dot(xc, wkb[slot], preferred_element_type=f32)
        acc[:, q_half + kv_half:] += jnp.dot(xc, wvb[slot], preferred_element_type=f32)

        @pl.when(j + RING < steps)
        def _():
            for c in weight_copies(j + RING, slot):
                c.start()

        @pl.when(j + RING >= steps)
        def _():
            out_copy(j + RING - steps).start()

    for s in range(RING, OUT_SLOTS):
        out_copy(s).start()

    for hh in range(my_heads * group):
        tl, g = hh // group, hh % group
        block = acc[:, hh * dim:(hh + 1) * dim].astype(bf16)
        for r in range(CORES):
            qsend[r, tl, g * rows:(g + 1) * rows, :] = block[r * rows:(r + 1) * rows]
    for part in range(2):
        for hl in range(my_heads):
            lo = q_half + part * kv_half + hl * dim
            block = acc[:, lo:lo + dim].astype(bf16)
            for r in range(CORES):
                knv_send[r, part, hl * rows:(hl + 1) * rows, :] = block[r * rows:(r + 1) * rows]

    def sib_copies():
        return [
            pltpu.make_async_remote_copy(qsend.at[1 - core], qsib, sib_ssem.at[0], sib_rsem.at[0], device_id={'ctx': sib}, device_id_type=MESH),
            pltpu.make_async_remote_copy(knv_send.at[1 - core], knv_recv, sib_ssem.at[1], sib_rsem.at[1], device_id={'ctx': sib}, device_id_type=MESH),
        ]

    for c in sib_copies():
        c.start()

    def place(step):
        return pl.ds(pl.multiple_of(step * qrows, 16), qrows)

    def q_copy(step, src):
        t = head_of(step)
        return pltpu.make_async_remote_copy(src.at[lax.rem(t, my_heads)], qrecv.at[place(step), :], q_ssem.at[step], q_rsem.at[step],
                                            device_id={'ctx': t * CORES + core}, device_id_type=MESH)

    def send_queries(half, src):
        @pl.when(chip // my_heads == half)
        def _():
            qrecv[0:qrows, :] = src[lax.rem(chip, my_heads)]

        @pl.loop(1, chips)
        def _(step):
            @pl.when(head_of(step) // my_heads == half)
            def _():
                q_copy(step, src).start()


    own = qsend[core].reshape(my_heads * qrows, dim).astype(f32)
    q32[pl.ds(pl.multiple_of(core * my_heads * qrows, 8), my_heads * qrows), :] = own
    own_kv = knv_send[core].astype(f32)
    own_at = pl.ds(pl.multiple_of(core * my_heads * rows, 8), my_heads * rows)
    kn32[own_at, :] = own_kv[0]
    vn32[own_at, :] = own_kv[1]
    for c in sib_copies():
        c.wait()
    sib_at = 1 - core
    q32[pl.ds(pl.multiple_of(sib_at * my_heads * qrows, 8), my_heads * qrows), :] = qsib[...].reshape(my_heads * qrows, dim).astype(f32)
    sib_kv = knv_recv[...].astype(f32)
    other = pl.ds(pl.multiple_of(sib_at * my_heads * rows, 8), my_heads * rows)
    kn32[other, :] = sib_kv[0]
    vn32[other, :] = sib_kv[1]

    first[3].wait()
    first[4].wait()
    n_q = heads * group
    row_id = lax.broadcasted_iota(jnp.int32, (n_q, slots * heads), 0)
    col_id = lax.broadcasted_iota(jnp.int32, (n_q, slots * heads), 1)
    low = (col_id & (heads - 1)) * group
    same_head = jnp.logical_and(row_id >= low, row_id < low + group)
    slot_of = col_id >> int(math.log2(heads))
    slot3 = lax.broadcasted_iota(jnp.int32, (slots, heads, dim), 0)

    @pl.loop(0, rows // UNROLL)
    def _(i):
        for u in range(UNROLL):
            b = i * UNROLL + u
            length = lens[b]
            qb = q32[pl.ds(b, n_q, stride=rows), :].astype(bf16)
            hit = slot3 == length
            kb = jnp.where(hit, kn32[pl.ds(b, heads, stride=rows), :][None], ksuf[b].astype(f32).reshape(slots, heads, dim))
            vb = jnp.where(hit, vn32[pl.ds(b, heads, stride=rows), :][None], vsuf[b].astype(f32).reshape(slots, heads, dim))
            kb = kb.reshape(slots * heads, dim).astype(bf16)
            vb = vb.reshape(slots * heads, dim).astype(bf16)
            ksuf[b] = kb
            vsuf[b] = vb
            s = lax.dot_general(qb, kb, (((1,), (1,)), ((), ())), preferred_element_type=f32)
            live = jnp.logical_and(same_head, slot_of <= length)
            s = jnp.where(live, s, -jnp.inf)
            m = s.max(axis=-1, keepdims=True)
            p = jnp.where(live, jnp.exp2((s - m) * base2), 0.0)
            l = p.sum(axis=-1, keepdims=True)
            ob = jnp.dot(p.astype(bf16), vb, preferred_element_type=f32)
            at = pl.ds(b, n_q, stride=rows)
            suf_o[at, :] = ob
            suf_m[at, :] = jnp.broadcast_to(m * base2, (n_q, dim))
            suf_l[at, :] = jnp.broadcast_to(l, (n_q, dim))

    cache_out = [pltpu.make_async_copy(ksuf, ks_out, out_sem.at[0]), pltpu.make_async_copy(vsuf, vs_out, out_sem.at[1])]
    for c in cache_out:
        c.start()

    for step in range(1, chips):
        kv_copy(near_of(step)).wait_send()
    send_queries(core, qsend.at[core])
    send_queries(1 - core, qsib)

    for step in range(1, chips):
        kv_arrival(near_of(step) * CORES + core).wait_recv()
        fw_copy(step).start()
    for c in range(chips):
        kv_arrival(c * CORES + 1 - core).wait_recv()

    def o_copy(step):
        return pltpu.make_async_remote_copy(osend.at[place(step), :], orecv.at[step], o_ssem.at[step], o_rsem.at[step],
                                            device_id={'ctx': home_of(step) * CORES + core}, device_id_type=MESH)

    def l_copy(step):
        at = step * qrows // dim
        return pltpu.make_async_remote_copy(lsend.at[pl.ds(at, 2)], lrecv.at[step], l_ssem.at[step], l_rsem.at[step],
                                            device_id={'ctx': home_of(step) * CORES + core}, device_id_type=MESH)

    def scores(tile, s, top):
        q = qrecv[tile * TILE:(tile + 1) * TILE, :]
        sc = lax.dot_general(kvrecv[s, 0], q, (((1,), (1,)), ((), ())), preferred_element_type=f32)
        scr[tile % 2, s] = sc
        return jnp.maximum(top, sc.reshape(pre // 8, 8, TILE).max(axis=0))

    def values(tile, s, m, mass, o):
        p = jnp.exp2(scr[tile % 2, s] * base2 - m)
        mass += p.reshape(pre // 8, 8, TILE).sum(axis=0)
        vt = jnp.concatenate([kvrecv[s, 1, lo:lo + dim, :] for lo in range(0, pre, dim)], axis=1)
        return mass, o + jnp.dot(vt, p.astype(bf16), preferred_element_type=f32)

    lowest = jnp.full((8, TILE), -jnp.inf, f32)
    tiles = chips * qrows // TILE
    row_of = lax.broadcasted_iota(jnp.int32, (qrows, 2 * dim), 0)
    lane_of = lax.broadcasted_iota(jnp.int32, (qrows, 2 * dim), 1)
    oacc[...] = jnp.zeros_like(oacc)

    def home(step):
        if not isinstance(step, int):
            o_copy(step).wait_recv()
            l_copy(step).wait_recv()

        t = head_of(step)
        line = jnp.concatenate([lrecv[step, 0], lrecv[step, 1]], axis=1)
        pick = lane_of == row_of + lax.rem(step * qrows, dim)
        lse = jnp.where(pick, jnp.broadcast_to(line, (qrows, 2 * dim)), 0.0).sum(axis=-1, keepdims=True)
        at = pl.ds(pl.multiple_of(t * qrows, 8), qrows)
        sm = suf_m[at, :]
        top = jnp.maximum(lse, sm)
        wp = jnp.exp2(lse - top)
        ws = jnp.exp2(sm - top)
        o = (wp * orecv[step].astype(f32) + ws * suf_o[at, :]) / (wp + ws * suf_l[at, :])
        o = o.astype(bf16)
        att = jnp.concatenate([o[g * rows:(g + 1) * rows] for g in range(group)], axis=1)
        out_copy(step).wait()
        slot = lax.rem(step, OUT_SLOTS)
        for b in range(0, model, 512):
            oacc[:, b:b + 512] += jnp.dot(att, wob[slot, :, b:b + 512], preferred_element_type=f32)

        @pl.when(step + OUT_SLOTS < chips)
        def _():
            out_copy(step + OUT_SLOTS).start()

    tops = None
    arrived = 0
    sent = 0
    for tile in range(tiles + 1):
        if tile < tiles:
            while arrived * qrows < (tile + 1) * TILE:
                if arrived > 0:
                    q_copy(arrived, qsib).wait_recv()
                arrived += 1
        m = None if tile == 0 else tops.max(axis=0, keepdims=True) * base2
        tops = lowest
        mass = jnp.zeros((8, TILE), f32)
        o = jnp.zeros((dim, TILE), f32)
        for s in range(n):
            if tile < tiles:
                tops = scores(tile, s, tops)
            if tile > 0:
                mass, o = values(tile - 1, s, m, mass, o)
        if tile > 0:
            done = tile - 1
            l = mass.sum(axis=0, keepdims=True)
            o = o / l
            lse = m + jnp.log2(l)
            osend[done * TILE:(done + 1) * TILE, :] = o.T.astype(bf16)
            for lo in range(0, TILE, dim):
                lsend[(done * TILE + lo) // dim] = lse[:, lo:lo + dim]
            while (sent + 1) * qrows <= (done + 1) * TILE:
                if sent == 0:
                    orecv[0] = osend[0:qrows, :]
                    lrecv[0] = lsend[0:2]
                else:
                    o_copy(sent).start()
                    l_copy(sent).start()
                sent += 1
            if done == 2:
                home(0)

    pl.loop(1, chips)(home)
    out_ref[...] = (x2[core].astype(f32) + oacc[...].astype(bf16).astype(f32)).astype(bf16)

    for step in range(chips):
        fw_copy(step).wait_send()

    @pl.loop(1, chips)
    def _(step):
        q_copy(step, qsib).wait_send()
        o_copy(step).wait_send()
        l_copy(step).wait_send()

    for c in cache_out:
        c.wait()


def publish_kernel(ins, outs, bufs, in_sem, out_sem):
    pieces = []
    for a in range(3):
        count = PIECES if a else 1
        size = ins[a].shape[0] // count
        for i in range(count):
            at = pl.ds(i * size, size)
            k = len(pieces)
            pieces.append((pltpu.make_async_copy(ins[a].at[at], bufs[a].at[at], in_sem.at[k]),
                           pltpu.make_async_copy(bufs[a].at[at], outs[a].at[at], out_sem.at[k])))
    for c, _ in pieces:
        c.start()
    for c, d in pieces:
        c.wait()
        d.start()
    for _, d in pieces:
        d.wait()


def publish(arrays):
    any_spec = pl.BlockSpec(memory_space=pl.ANY)
    count = 1 + 2 * PIECES

    def kernel(a, b, c, x, y, z, p, q, r, in_sem, out_sem):
        publish_kernel((a, b, c), (x, y, z), (p, q, r), in_sem, out_sem)

    return pl.pallas_call(
        kernel,
        out_shape=tuple(jax.ShapeDtypeStruct(a.shape, a.dtype) for a in arrays),
        in_specs=[any_spec] * 3,
        out_specs=(any_spec,) * 3,
        scratch_shapes=[pltpu.VMEM(a.shape, a.dtype) for a in arrays] + [pltpu.SemaphoreType.DMA((count,))] * 2,
        compiler_params=pltpu.CompilerParams(vmem_limit_bytes=67_043_328),
    )(*arrays)


def solution(mesh):
    n = mesh.shape['ctx']
    home_axes = ('data', 'ctx')
    row_spec = P(home_axes, None)
    lens_spec = P(home_axes)
    whole_spec = P()
    prefix_spec = P(None, home_axes, None, None)
    cache_spec = P(None, home_axes, None, None, None)
    bf16, f32 = jnp.bfloat16, jnp.float32

    def attend(hidden, seq_lens, wq, wk, wv, wo, kp, vp, ks, vs):
        rows, model = hidden.shape
        _, pre, heads, dim = kp.shape
        slots = ks.shape[2]
        group = wq.shape[2] // (heads * dim)
        chips = n // CORES
        my_heads = heads // CORES
        qrows = group * rows
        qw = heads * group * dim
        dims = (rows, model, heads, group, dim, slots, pre)
        dma = pltpu.SemaphoreType.DMA
        vmem = pltpu.VMEM
        scratch = [
            vmem((CORES, rows, model), bf16),
            vmem((RING, CHUNK, qw // CORES), bf16),
            vmem((RING, CHUNK, heads * dim // CORES), bf16),
            vmem((RING, CHUNK, heads * dim // CORES), bf16),
            vmem((OUT_SLOTS, qw // chips, model), bf16),
            vmem((pre * heads, dim), bf16),
            vmem((pre * heads, dim), bf16),
            vmem((pre * heads, dim), f32),
            vmem((heads, 2, pre, dim), bf16),
            vmem((n, 2, pre, dim), bf16),
            vmem((CORES * rows, (qw + 2 * heads * dim) // CORES), f32),
            vmem((CORES, my_heads, qrows, dim), bf16),
            vmem((chips * qrows, dim), bf16),
            vmem((my_heads, qrows, dim), bf16),
            vmem((CORES, 2, my_heads * rows, dim), bf16),
            vmem((2, my_heads * rows, dim), bf16),
            vmem((heads * qrows, dim), f32),
            vmem((heads * rows, dim), f32),
            vmem((heads * rows, dim), f32),
            vmem((rows, slots * heads, dim), bf16),
            vmem((rows, slots * heads, dim), bf16),
            vmem((heads * qrows, dim), f32),
            vmem((heads * qrows, dim), f32),
            vmem((heads * qrows, dim), f32),
            vmem((2, n, pre, TILE), f32),
            vmem((chips * qrows, dim), bf16),
            vmem((chips * qrows // dim, 1, dim), f32),
            vmem((chips, qrows, dim), bf16),
            vmem((chips, 2, 1, dim), f32),
            vmem((rows, model), f32),
            pltpu.SemaphoreType.REGULAR((chips,)),
            dma((5,)),
            dma((2,)),
            dma((RING, 3)),
            dma((OUT_SLOTS,)),
            dma,
            dma,
            dma((chips,)),
            dma((n,)),
            dma((chips,)),
            dma((chips,)),
            dma((chips,)),
            dma((2,)),
            dma((2,)),
            dma((chips,)),
            dma((chips,)),
            dma((chips,)),
            dma((chips,)),
        ]
        any_spec = pl.BlockSpec(memory_space=pl.ANY)
        vmem_spec = pl.BlockSpec(memory_space=pltpu.VMEM)
        return pl.pallas_call(
            functools.partial(decode_kernel, n, dims),
            out_shape=(jax.ShapeDtypeStruct((rows, model), bf16),) + (jax.ShapeDtypeStruct((rows, slots * heads, dim), bf16),) * 2,
            in_specs=[pl.BlockSpec(memory_space=pltpu.SMEM)] + [any_spec] * 9,
            out_specs=(vmem_spec, any_spec, any_spec),
            scratch_shapes=scratch,
            compiler_params=pltpu.CompilerParams(collective_id=0, has_side_effects=True, vmem_limit_bytes=67_043_328),
        )(seq_lens, hidden, wq, wk, wv, wo, kp.reshape(pre * heads, dim), vp.reshape(pre * heads, dim),
          ks.reshape(rows, slots * heads, dim), vs.reshape(rows, slots * heads, dim))

    def local_step(hidden, seq_lens, wq, wk, wv, wo, kp, vp, ks, vs):
        out, k_new, v_new = publish(attend(hidden, seq_lens, wq, wk, wv, wo, kp, vp, ks, vs))
        return out, k_new.reshape(ks.shape), v_new.reshape(vs.shape)

    return jax.shard_map(local_step, mesh=mesh, in_specs=(row_spec, lens_spec, whole_spec, whole_spec, whole_spec, whole_spec, prefix_spec, prefix_spec, cache_spec, cache_spec), out_specs=(row_spec, cache_spec, cache_spec), check_vma=False)
```

```python
import functools
import math

import jax
import jax.numpy as jnp
from jax import lax
from jax.experimental import pallas as pl
from jax.experimental.pallas import tpu as pltpu
from jax.sharding import PartitionSpec as P

MESH = pl.DeviceIdType.MESH
CORES = 2
CHUNK = 256
RING = 4
OUT_SLOTS = 5
TILE = 256

UNROLL = 4
PIECES = 8


def hop_of(step):
    return (step + 1) // 2 * (1 - 2 * ((step + 1) % 2))


def decode_kernel(n, dims, lens, x_hbm, wq, wk, wv, wo, kp, vp, ks_hbm, vs_hbm, out_ref, ks_out, vs_out,
                  x2, wqb, wkb, wvb, wob, kraw, vraw, tmp, kvsend, kvrecv, acc, qsend, qrecv, qsib, knv_send, knv_recv,
                  q32, kn32, vn32, ksuf, vsuf, suf_o, suf_m, suf_l, scr, osend, lsend, orecv, lrecv, oacc,
                  up_sem, in_sem, out_sem, wsem, wosem, x_ssem, x_rsem, kv_ssem, kv_rsem, fw_ssem, q_ssem, q_rsem, sib_ssem, sib_rsem,
                  o_ssem, o_rsem, l_ssem, l_rsem):
    rows, model, heads, group, dim, slots, pre = dims
    chips = n // CORES
    qw = heads * group * dim
    q_half = qw // CORES
    kv_half = heads * dim // CORES
    my_heads = heads // CORES
    qrows = group * rows
    base2 = dim ** -0.5 * math.log2(math.e)
    me = lax.axis_index('ctx')
    chip = me // CORES
    core = me % CORES
    sib = me + 1 - 2 * core
    f32, bf16 = jnp.float32, jnp.bfloat16
    steps = model // CHUNK
    out_rows = qw // chips

    def loads():
        return [
            pltpu.make_async_copy(kp, kraw, in_sem.at[0]),
            pltpu.make_async_copy(vp, vraw, in_sem.at[1]),
            pltpu.make_async_copy(x_hbm, x2.at[core], in_sem.at[2]),
            pltpu.make_async_copy(ks_hbm, ksuf, in_sem.at[3]),
            pltpu.make_async_copy(vs_hbm, vsuf, in_sem.at[4]),
        ]

    def weight_copies(step, slot):
        r = pl.ds(pl.multiple_of(step * CHUNK, CHUNK), CHUNK)
        qc = pl.ds(pl.multiple_of(core * q_half, 128), q_half)
        kc = pl.ds(pl.multiple_of(core * kv_half, 128), kv_half)
        return [
            pltpu.make_async_copy(wq.at[0, r, qc], wqb.at[slot], wsem.at[slot, 0]),
            pltpu.make_async_copy(wk.at[0, r, kc], wkb.at[slot], wsem.at[slot, 1]),
            pltpu.make_async_copy(wv.at[0, r, kc], wvb.at[slot], wsem.at[slot, 2]),
        ]

    def home_of(step):
        return lax.rem(chip + hop_of(step) + chips, chips)

    def head_of(step):
        return lax.rem(chip - hop_of(step) + chips, chips)

    def near_of(step):
        return lax.rem(chip + (step + 1) // 2 * (1 - 2 * ((step + 1) % 2)) + chips, chips)

    def out_copy(step):
        slot = lax.rem(step, OUT_SLOTS)
        r = pl.ds(pl.multiple_of(head_of(step) * out_rows, out_rows), out_rows)
        return pltpu.make_async_copy(wo.at[0, r, :], wob.at[slot], wosem.at[slot])

    first = loads()
    for c in first[:2]:
        c.start()

    barrier = pltpu.get_barrier_semaphore()
    pl.semaphore_signal(barrier, inc=1, device_id={'ctx': sib}, device_id_type=MESH)
    for t in range(1, chips):
        @pl.when(t > chip)
        def _():
            for r in range(CORES):
                pl.semaphore_signal(barrier, inc=1, device_id={'ctx': t * CORES + r}, device_id_type=MESH)

    pl.semaphore_wait(barrier, chip * CORES + 1)
    for t in range(chips - 1):
        @pl.when(t < chip)
        def _():
            for r in range(CORES):
                pl.semaphore_signal(up_sem.at[chip], inc=1, device_id={'ctx': t * CORES + r}, device_id_type=MESH)

    for part, raw in ((0, kraw), (1, vraw)):
        first[part].wait()
        if part == 1:
            first[2].start()
            for s in range(RING):
                for c in weight_copies(s, s):
                    c.start()
            for c in first[3:]:
                c.start()
        tmp[...] = raw[...].astype(f32)
        for h in range(heads):
            block = tmp[pl.ds(h, pre, stride=heads), :]
            if part == 0:
                kvsend[h, 0] = block.astype(bf16)
            else:
                for lo in range(0, pre, dim):
                    kvsend[h, 1, lo:lo + dim, :] = block[lo:lo + dim].T.astype(bf16)
    kvrecv[me] = kvsend[chip]
    x_copy = pltpu.make_async_remote_copy(x2.at[core], x2.at[core], x_ssem, x_rsem, device_id={'ctx': sib}, device_id_type=MESH)

    def kv_copy(t):
        return pltpu.make_async_remote_copy(kvsend.at[t], kvrecv.at[me], kv_ssem.at[t], kv_rsem.at[me],
                                            device_id={'ctx': t * CORES + core}, device_id_type=MESH)

    def fw_copy(step):
        j = near_of(step) * CORES + core
        src = kvsend.at[chip] if step == 0 else kvrecv.at[j]
        return pltpu.make_async_remote_copy(src, kvrecv.at[j], fw_ssem.at[step], kv_rsem.at[j],
                                            device_id={'ctx': sib}, device_id_type=MESH)

    def kv_arrival(j):
        return pltpu.make_async_remote_copy(kvsend.at[0], kvrecv.at[j], kv_ssem.at[0], kv_rsem.at[j],
                                            device_id={'ctx': sib}, device_id_type=MESH)

    for step in range(1, chips):
        t = near_of(step)

        @pl.when(t > chip)
        def _():
            pl.semaphore_wait(up_sem.at[t], CORES)

        kv_copy(t).start()
    fw_copy(0).start()
    first[2].wait()
    x_copy.start()
    acc[...] = jnp.zeros_like(acc)
    x_copy.wait()

    @pl.loop(0, steps)
    def _(j):
        slot = lax.rem(j, RING)
        for c in weight_copies(j, slot):
            c.wait()
        xc = x2[:, :, pl.ds(pl.multiple_of(j * CHUNK, CHUNK), CHUNK)].reshape(CORES * rows, CHUNK)
        for b in range(0, q_half, 512):
            acc[:, b:b + 512] += jnp.dot(xc, wqb[slot, :, b:b + 512], preferred_element_type=f32)
        acc[:, q_half:q_half + kv_half] += jnp.dot(xc, wkb[slot], preferred_element_type=f32)
        acc[:, q_half + kv_half:] += jnp.dot(xc, wvb[slot], preferred_element_type=f32)

        @pl.when(j + RING < steps)
        def _():
            for c in weight_copies(j + RING, slot):
                c.start()

        @pl.when(j + RING >= steps)
        def _():
            out_copy(j + RING - steps).start()

    for s in range(RING, OUT_SLOTS):
        out_copy(s).start()

    for hh in range(my_heads * group):
        tl, g = hh // group, hh % group
        block = acc[:, hh * dim:(hh + 1) * dim].astype(bf16)
        for r in range(CORES):
            qsend[r, tl, g * rows:(g + 1) * rows, :] = block[r * rows:(r + 1) * rows]
    for part in range(2):
        for hl in range(my_heads):
            lo = q_half + part * kv_half + hl * dim
            block = acc[:, lo:lo + dim].astype(bf16)
            for r in range(CORES):
                knv_send[r, part, hl * rows:(hl + 1) * rows, :] = block[r * rows:(r + 1) * rows]

    def sib_copies():
        return [
            pltpu.make_async_remote_copy(qsend.at[1 - core], qsib, sib_ssem.at[0], sib_rsem.at[0], device_id={'ctx': sib}, device_id_type=MESH),
            pltpu.make_async_remote_copy(knv_send.at[1 - core], knv_recv, sib_ssem.at[1], sib_rsem.at[1], device_id={'ctx': sib}, device_id_type=MESH),
        ]

    for c in sib_copies():
        c.start()

    def place(step):
        return pl.ds(pl.multiple_of(step * qrows, 16), qrows)

    def q_copy(step, src):
        t = head_of(step)
        return pltpu.make_async_remote_copy(src.at[lax.rem(t, my_heads)], qrecv.at[place(step), :], q_ssem.at[step], q_rsem.at[step],
                                            device_id={'ctx': t * CORES + core}, device_id_type=MESH)

    def send_queries(half, src):
        @pl.when(chip // my_heads == half)
        def _():
            qrecv[0:qrows, :] = src[lax.rem(chip, my_heads)]

        @pl.loop(1, chips)
        def _(step):
            @pl.when(head_of(step) // my_heads == half)
            def _():
                q_copy(step, src).start()


    own = qsend[core].reshape(my_heads * qrows, dim).astype(f32)
    q32[pl.ds(pl.multiple_of(core * my_heads * qrows, 8), my_heads * qrows), :] = own
    own_kv = knv_send[core].astype(f32)
    own_at = pl.ds(pl.multiple_of(core * my_heads * rows, 8), my_heads * rows)
    kn32[own_at, :] = own_kv[0]
    vn32[own_at, :] = own_kv[1]
    for c in sib_copies():
        c.wait()
    sib_at = 1 - core
    q32[pl.ds(pl.multiple_of(sib_at * my_heads * qrows, 8), my_heads * qrows), :] = qsib[...].reshape(my_heads * qrows, dim).astype(f32)
    sib_kv = knv_recv[...].astype(f32)
    other = pl.ds(pl.multiple_of(sib_at * my_heads * rows, 8), my_heads * rows)
    kn32[other, :] = sib_kv[0]
    vn32[other, :] = sib_kv[1]

    first[3].wait()
    first[4].wait()
    n_q = heads * group
    row_id = lax.broadcasted_iota(jnp.int32, (n_q, slots * heads), 0)
    col_id = lax.broadcasted_iota(jnp.int32, (n_q, slots * heads), 1)
    low = (col_id & (heads - 1)) * group
    same_head = jnp.logical_and(row_id >= low, row_id < low + group)
    slot_of = col_id >> int(math.log2(heads))
    slot3 = lax.broadcasted_iota(jnp.int32, (slots, heads, dim), 0)

    def suffix(i):
        for u in range(UNROLL):
            b = i * UNROLL + u
            length = lens[b]
            qb = q32[pl.ds(b, n_q, stride=rows), :].astype(bf16)
            hit = slot3 == length
            kb = jnp.where(hit, kn32[pl.ds(b, heads, stride=rows), :][None], ksuf[b].astype(f32).reshape(slots, heads, dim))
            vb = jnp.where(hit, vn32[pl.ds(b, heads, stride=rows), :][None], vsuf[b].astype(f32).reshape(slots, heads, dim))
            kb = kb.reshape(slots * heads, dim).astype(bf16)
            vb = vb.reshape(slots * heads, dim).astype(bf16)
            ksuf[b] = kb
            vsuf[b] = vb
            s = lax.dot_general(qb, kb, (((1,), (1,)), ((), ())), preferred_element_type=f32)
            live = jnp.logical_and(same_head, slot_of <= length)
            s = jnp.where(live, s, -jnp.inf)
            m = s.max(axis=-1, keepdims=True)
            p = jnp.where(live, jnp.exp2((s - m) * base2), 0.0)
            l = p.sum(axis=-1, keepdims=True)
            ob = jnp.dot(p.astype(bf16), vb, preferred_element_type=f32)
            at = pl.ds(b, n_q, stride=rows)
            suf_o[at, :] = ob
            suf_m[at, :] = jnp.broadcast_to(m * base2, (n_q, dim))
            suf_l[at, :] = jnp.broadcast_to(l, (n_q, dim))

    early = rows // UNROLL * 3 // 4
    pl.loop(0, early)(suffix)
    send_queries(core, qsend.at[core])
    send_queries(1 - core, qsib)
    pl.loop(early, rows // UNROLL)(suffix)

    cache_out = [pltpu.make_async_copy(ksuf, ks_out, out_sem.at[0]), pltpu.make_async_copy(vsuf, vs_out, out_sem.at[1])]
    for c in cache_out:
        c.start()

    for step in range(1, chips):
        kv_arrival(near_of(step) * CORES + core).wait_recv()
        fw_copy(step).start()
    for c in range(chips):
        kv_arrival(c * CORES + 1 - core).wait_recv()

    def o_copy(step):
        return pltpu.make_async_remote_copy(osend.at[place(step), :], orecv.at[step], o_ssem.at[step], o_rsem.at[step],
                                            device_id={'ctx': home_of(step) * CORES + core}, device_id_type=MESH)

    def l_copy(step):
        at = step * qrows // dim
        return pltpu.make_async_remote_copy(lsend.at[pl.ds(at, 2)], lrecv.at[step], l_ssem.at[step], l_rsem.at[step],
                                            device_id={'ctx': home_of(step) * CORES + core}, device_id_type=MESH)

    def scores(tile, s, top):
        q = qrecv[tile * TILE:(tile + 1) * TILE, :]
        sc = lax.dot_general(kvrecv[s, 0], q, (((1,), (1,)), ((), ())), preferred_element_type=f32)
        scr[tile % 2, s] = sc
        return jnp.maximum(top, sc.reshape(pre // 8, 8, TILE).max(axis=0))

    def values(tile, s, m, mass, o):
        p = jnp.exp2(scr[tile % 2, s] * base2 - m)
        mass += p.reshape(pre // 8, 8, TILE).sum(axis=0)
        vt = jnp.concatenate([kvrecv[s, 1, lo:lo + dim, :] for lo in range(0, pre, dim)], axis=1)
        return mass, o + jnp.dot(vt, p.astype(bf16), preferred_element_type=f32)

    lowest = jnp.full((8, TILE), -jnp.inf, f32)
    tiles = chips * qrows // TILE
    row_of = lax.broadcasted_iota(jnp.int32, (qrows, 2 * dim), 0)
    lane_of = lax.broadcasted_iota(jnp.int32, (qrows, 2 * dim), 1)
    oacc[...] = jnp.zeros_like(oacc)

    def home(step):
        if not isinstance(step, int):
            o_copy(step).wait_recv()
            l_copy(step).wait_recv()

        t = head_of(step)
        line = jnp.concatenate([lrecv[step, 0], lrecv[step, 1]], axis=1)
        pick = lane_of == row_of + lax.rem(step * qrows, dim)
        lse = jnp.where(pick, jnp.broadcast_to(line, (qrows, 2 * dim)), 0.0).sum(axis=-1, keepdims=True)
        at = pl.ds(pl.multiple_of(t * qrows, 8), qrows)
        sm = suf_m[at, :]
        top = jnp.maximum(lse, sm)
        wp = jnp.exp2(lse - top)
        ws = jnp.exp2(sm - top)
        o = (wp * orecv[step].astype(f32) + ws * suf_o[at, :]) / (wp + ws * suf_l[at, :])
        o = o.astype(bf16)
        att = jnp.concatenate([o[g * rows:(g + 1) * rows] for g in range(group)], axis=1)
        out_copy(step).wait()
        slot = lax.rem(step, OUT_SLOTS)
        for b in range(0, model, 512):
            oacc[:, b:b + 512] += jnp.dot(att, wob[slot, :, b:b + 512], preferred_element_type=f32)

        @pl.when(step + OUT_SLOTS < chips)
        def _():
            out_copy(step + OUT_SLOTS).start()

    tops = None
    arrived = 0
    sent = 0
    for tile in range(tiles + 1):
        if tile < tiles:
            while arrived * qrows < (tile + 1) * TILE:
                if arrived > 0:
                    q_copy(arrived, qsib).wait_recv()
                arrived += 1
        m = None if tile == 0 else tops.max(axis=0, keepdims=True) * base2
        tops = lowest
        mass = jnp.zeros((8, TILE), f32)
        o = jnp.zeros((dim, TILE), f32)
        for s in range(n):
            if tile < tiles:
                tops = scores(tile, s, tops)
            if tile > 0:
                mass, o = values(tile - 1, s, m, mass, o)
        if tile > 0:
            done = tile - 1
            l = mass.sum(axis=0, keepdims=True)
            o = o / l
            lse = m + jnp.log2(l)
            osend[done * TILE:(done + 1) * TILE, :] = o.T.astype(bf16)
            for lo in range(0, TILE, dim):
                lsend[(done * TILE + lo) // dim] = lse[:, lo:lo + dim]
            while (sent + 1) * qrows <= (done + 1) * TILE:
                if sent == 0:
                    orecv[0] = osend[0:qrows, :]
                    lrecv[0] = lsend[0:2]
                else:
                    o_copy(sent).start()
                    l_copy(sent).start()
                sent += 1

    home(0)
    pl.loop(1, chips)(home)
    out_ref[...] = (x2[core].astype(f32) + oacc[...].astype(bf16).astype(f32)).astype(bf16)

    for step in range(1, chips):
        kv_copy(near_of(step)).wait_send()
    for step in range(chips):
        fw_copy(step).wait_send()

    @pl.loop(1, chips)
    def _(step):
        q_copy(step, qsib).wait_send()
        o_copy(step).wait_send()
        l_copy(step).wait_send()

    for c in cache_out:
        c.wait()


def publish_kernel(ins, outs, bufs, in_sem, out_sem):
    pieces = []
    for a in range(3):
        count = PIECES if a else 1
        size = ins[a].shape[0] // count
        for i in range(count):
            at = pl.ds(i * size, size)
            k = len(pieces)
            pieces.append((pltpu.make_async_copy(ins[a].at[at], bufs[a].at[at], in_sem.at[k]),
                           pltpu.make_async_copy(bufs[a].at[at], outs[a].at[at], out_sem.at[k])))
    for c, _ in pieces:
        c.start()
    for c, d in pieces:
        c.wait()
        d.start()
    for _, d in pieces:
        d.wait()


def publish(arrays):
    any_spec = pl.BlockSpec(memory_space=pl.ANY)
    count = 1 + 2 * PIECES

    def kernel(a, b, c, x, y, z, p, q, r, in_sem, out_sem):
        publish_kernel((a, b, c), (x, y, z), (p, q, r), in_sem, out_sem)

    return pl.pallas_call(
        kernel,
        out_shape=tuple(jax.ShapeDtypeStruct(a.shape, a.dtype) for a in arrays),
        in_specs=[any_spec] * 3,
        out_specs=(any_spec,) * 3,
        scratch_shapes=[pltpu.VMEM(a.shape, a.dtype) for a in arrays] + [pltpu.SemaphoreType.DMA((count,))] * 2,
        compiler_params=pltpu.CompilerParams(vmem_limit_bytes=67_043_328),
    )(*arrays)


def solution(mesh):
    n = mesh.shape['ctx']
    home_axes = ('data', 'ctx')
    row_spec = P(home_axes, None)
    lens_spec = P(home_axes)
    whole_spec = P()
    prefix_spec = P(None, home_axes, None, None)
    cache_spec = P(None, home_axes, None, None, None)
    bf16, f32 = jnp.bfloat16, jnp.float32

    def attend(hidden, seq_lens, wq, wk, wv, wo, kp, vp, ks, vs):
        rows, model = hidden.shape
        _, pre, heads, dim = kp.shape
        slots = ks.shape[2]
        group = wq.shape[2] // (heads * dim)
        chips = n // CORES
        my_heads = heads // CORES
        qrows = group * rows
        qw = heads * group * dim
        dims = (rows, model, heads, group, dim, slots, pre)
        dma = pltpu.SemaphoreType.DMA
        vmem = pltpu.VMEM
        scratch = [
            vmem((CORES, rows, model), bf16),
            vmem((RING, CHUNK, qw // CORES), bf16),
            vmem((RING, CHUNK, heads * dim // CORES), bf16),
            vmem((RING, CHUNK, heads * dim // CORES), bf16),
            vmem((OUT_SLOTS, qw // chips, model), bf16),
            vmem((pre * heads, dim), bf16),
            vmem((pre * heads, dim), bf16),
            vmem((pre * heads, dim), f32),
            vmem((heads, 2, pre, dim), bf16),
            vmem((n, 2, pre, dim), bf16),
            vmem((CORES * rows, (qw + 2 * heads * dim) // CORES), f32),
            vmem((CORES, my_heads, qrows, dim), bf16),
            vmem((chips * qrows, dim), bf16),
            vmem((my_heads, qrows, dim), bf16),
            vmem((CORES, 2, my_heads * rows, dim), bf16),
            vmem((2, my_heads * rows, dim), bf16),
            vmem((heads * qrows, dim), f32),
            vmem((heads * rows, dim), f32),
            vmem((heads * rows, dim), f32),
            vmem((rows, slots * heads, dim), bf16),
            vmem((rows, slots * heads, dim), bf16),
            vmem((heads * qrows, dim), f32),
            vmem((heads * qrows, dim), f32),
            vmem((heads * qrows, dim), f32),
            vmem((2, n, pre, TILE), f32),
            vmem((chips * qrows, dim), bf16),
            vmem((chips * qrows // dim, 1, dim), f32),
            vmem((chips, qrows, dim), bf16),
            vmem((chips, 2, 1, dim), f32),
            vmem((rows, model), f32),
            pltpu.SemaphoreType.REGULAR((chips,)),
            dma((5,)),
            dma((2,)),
            dma((RING, 3)),
            dma((OUT_SLOTS,)),
            dma,
            dma,
            dma((chips,)),
            dma((n,)),
            dma((chips,)),
            dma((chips,)),
            dma((chips,)),
            dma((2,)),
            dma((2,)),
            dma((chips,)),
            dma((chips,)),
            dma((chips,)),
            dma((chips,)),
        ]
        any_spec = pl.BlockSpec(memory_space=pl.ANY)
        vmem_spec = pl.BlockSpec(memory_space=pltpu.VMEM)
        return pl.pallas_call(
            functools.partial(decode_kernel, n, dims),
            out_shape=(jax.ShapeDtypeStruct((rows, model), bf16),) + (jax.ShapeDtypeStruct((rows, slots * heads, dim), bf16),) * 2,
            in_specs=[pl.BlockSpec(memory_space=pltpu.SMEM)] + [any_spec] * 9,
            out_specs=(vmem_spec, any_spec, any_spec),
            scratch_shapes=scratch,
            compiler_params=pltpu.CompilerParams(collective_id=0, has_side_effects=True, vmem_limit_bytes=67_043_328),
        )(seq_lens, hidden, wq, wk, wv, wo, kp.reshape(pre * heads, dim), vp.reshape(pre * heads, dim),
          ks.reshape(rows, slots * heads, dim), vs.reshape(rows, slots * heads, dim))

    def local_step(hidden, seq_lens, wq, wk, wv, wo, kp, vp, ks, vs):
        out, k_new, v_new = publish(attend(hidden, seq_lens, wq, wk, wv, wo, kp, vp, ks, vs))
        return out, k_new.reshape(ks.shape), v_new.reshape(vs.shape)

    return jax.shard_map(local_step, mesh=mesh, in_specs=(row_spec, lens_spec, whole_spec, whole_spec, whole_spec, whole_spec, prefix_spec, prefix_spec, cache_spec, cache_spec), out_specs=(row_spec, cache_spec, cache_spec), check_vma=False)
```
